32 devices in a mesh: wide: 8 (over z, y), narrow: 4 (over x, core).
Axes of the slice: x: 2, y: 2, z: 4, core: 2. Of those that a mesh axis runs over, the one named last changes fastest.
Arguments:
- tokens: bfloat16 [8192, 2304], P(('wide', 'narrow')), may hold values from -6 to 6
- norm_attn: bfloat16 [2304], replicated, may hold values from 0.25 to 1.75
- norm_ffn: bfloat16 [2304], replicated, may hold values from 0.25 to 1.75
- w_query: bfloat16 [2304, 2304], P('wide', 'narrow'), may hold values from -0.125 to 0.125
- w_key: bfloat16 [2304, 2304], P('wide', 'narrow'), may hold values from -0.125 to 0.125
- w_value: bfloat16 [2304, 2304], P('wide', 'narrow'), may hold values from -0.125 to 0.125
- w_out: bfloat16 [2304, 2304], P('narrow', 'wide'), may hold values from -3 to 3
- w_gate: bfloat16 [2304, 5760], P('wide', 'narrow'), may hold values from -0.125 to 0.125
- w_up: bfloat16 [2304, 5760], P('wide', 'narrow'), may hold values from -0.125 to 0.125
- w_down: bfloat16 [5760, 2304], P('narrow', 'wide'), may hold values from -0.625 to 0.625
- cotangent: bfloat16 [8192, 2304], P(('wide', 'narrow')), may hold values from -6 to 6
- lengths: int32 [2, 8], replicated, may hold values from 0 to 1024, as said below
- deal: int32 [1024], replicated, may hold values from 0 to 1023, as said below
Outputs:
- output: bfloat16 [8192, 2304], P(('wide', 'narrow'))
- grad_tokens: bfloat16 [8192, 2304], P(('wide', 'narrow'))
- grad_norm_attn: float32 [2304], replicated
- grad_norm_ffn: float32 [2304], replicated
- grad_query: float32 [2304, 2304], P('wide', 'narrow')
- grad_key: float32 [2304, 2304], P('wide', 'narrow')
- grad_value: float32 [2304, 2304], P('wide', 'narrow')
- grad_out: float32 [2304, 2304], P('narrow', 'wide')
- grad_gate: float32 [2304, 5760], P('wide', 'narrow')
- grad_up: float32 [2304, 5760], P('wide', 'narrow')
- grad_down: float32 [5760, 2304], P('narrow', 'wide')
The draws below stay inside these ranges and needn't reach their ends.
Inputs may be any that keep to these rules, and one draw needn't show every extreme that they name: Micro-batch 0: for each p, sequences 2p and 2p+1 fill stream rows 2p 512 to 2p 512 + 2 * 512 - 1 (their extents add up to 1024); sequence 0 has length 1024 and sequence 1 length 0. Micro-batch 1: sequence 0 has extent 512; for each p from 0 to 2, sequences 2p+1 and 2p+2 fill stream rows (2p+1) * 512 to (2p+3) * 512 - 1; the last sequence has extent 512; sequences 3 and 4 have lengths 1024 and 0. In both, the first sequence of each such pair has a length that is a multiple of 64. deal is a permutation of 0 .. 1023. Dealt block g and source block deal[g] lie on devices with the same index of narrow. For every two indices of wide, exactly 4 blocks of one device goes to the device with the other index of wide and the same index of narrow.
All inputs are finite; a program needn't handle non-finite values.
Results may differ from the reference program's by a relative error of at most 0.019.
Values may be sent and summed in bfloat16 or wider, within the bound.
A program may use at most 160 MiB of HBM per device.

```python
import math
import jax
import jax.numpy as jnp
from jax import lax

D = 2304
HEADS = 36
HEAD_DIM = 64
FF = 5760
TOK_DEV = 256
MB = 2
BLK = 8
UNIT = 64
RANKS = 8
LANES = 4
BLOCKS_DEV = 32
SLOT = 512
NBLK = 1024
TOKENS = 8192
N_WIDE = 8
N_NARROW = 4


def pair_lengths(key, count, unit_count, forced):
    first_key = jax.random.fold_in(key, 1)
    second_key = jax.random.fold_in(key, 2)
    split_units = jax.random.randint(first_key, (count,), 0, unit_count + 1)
    split_units = split_units.at[forced].set(unit_count)
    padding = jax.random.randint(second_key, (count,), 0, UNIT)
    first_len = split_units * UNIT
    second_extent = (unit_count - split_units) * UNIT
    second_len = jnp.maximum(second_extent - padding, 0)
    return jnp.stack([first_len, second_len], axis=1).reshape(-1)


def draw_lengths(key, part):
    pair_count = RANKS // 2
    unit_count = 2 * SLOT // UNIT
    row_first = pair_lengths(jax.random.fold_in(key, 11), pair_count, unit_count, 0)
    inner = pair_lengths(jax.random.fold_in(key, 12), pair_count - 1, unit_count, pair_count // 2 - 1)
    edge_pad = jax.random.randint(jax.random.fold_in(key, 13), (2,), 0, UNIT)
    edges = SLOT - edge_pad
    row_second = jnp.concatenate([edges[0:1], inner, edges[1:2]])
    return jnp.stack([row_first, row_second], axis=0).astype(jnp.int32)


def draw_deal(key, part):
    shift_key = jax.random.fold_in(key, 21)
    order_key = jax.random.fold_in(key, 22)
    offset = jax.random.randint(shift_key, (), 0, RANKS)
    keys_all = jax.random.split(order_key, RANKS * LANES)
    orders = jax.vmap(lambda one_key: jax.random.permutation(one_key, BLOCKS_DEV))(keys_all)
    orders = orders.reshape(RANKS, LANES, BLOCKS_DEV)
    dest_rank = jnp.arange(RANKS, dtype=jnp.int32)[:, None, None]
    lane_index = jnp.arange(LANES, dtype=jnp.int32)[None, :, None]
    slot_index = jnp.arange(BLOCKS_DEV, dtype=jnp.int32)[None, None, :]
    source_rank = (dest_rank + offset + slot_index) % RANKS
    local_index = orders[source_rank, lane_index, slot_index]
    dealt = (source_rank * LANES + lane_index) * BLOCKS_DEV + local_index
    return dealt.reshape(-1).astype(jnp.int32)


def shard_levels(key, dims, cuts, smallest, largest):
    level = 1.0
    for dim, blocks in cuts:
        heights = jax.random.uniform(jax.random.fold_in(jax.random.fold_in(key, 6), dim), (blocks,), jnp.float32, smallest / len(cuts), largest / len(cuts))
        level = level * jnp.repeat(jnp.exp(heights), dims[dim] // blocks).reshape((-1,) + (1,) * (len(dims) - 1 - dim))
    return level


def gaussian(rng, dims, width, limit, cuts=(), kind=jnp.bfloat16):
    values = width * jax.random.normal(rng, dims, jnp.float32)
    if cuts:
        values = values * shard_levels(rng, dims, cuts, -0.22, 0.18)
    return jnp.clip(values, -limit, limit).astype(kind)


def setup_inputs(seed: int = 0) -> dict:
    key_list = jax.random.split(jax.random.key(seed), 14)
    tokens = gaussian(key_list[0], (TOKENS, D), 1.0, 6.0, ((0, 32),))
    norm_attn = jnp.clip(1.0 + 0.15 * jax.random.normal(key_list[1], (D,), jnp.float32), 0.25, 1.75).astype(jnp.bfloat16)
    norm_ffn = jnp.clip(1.0 + 0.15 * jax.random.normal(key_list[2], (D,), jnp.float32), 0.25, 1.75).astype(jnp.bfloat16)
    w_query = gaussian(key_list[3], (D, D), D ** -0.5, 0.125, ((0, 8), (1, 4)))
    w_key = gaussian(key_list[4], (D, D), D ** -0.5, 0.125, ((0, 8), (1, 4)))
    w_value = gaussian(key_list[5], (D, D), D ** -0.5, 0.125, ((0, 8), (1, 4)))
    w_out = gaussian(key_list[6], (D, D), 0.5, 3.0, ((0, 4), (1, 8)))
    w_gate = gaussian(key_list[7], (D, FF), D ** -0.5, 0.125, ((0, 8), (1, 4)))
    w_up = gaussian(key_list[8], (D, FF), D ** -0.5, 0.125, ((0, 8), (1, 4)))
    w_down = gaussian(key_list[9], (FF, D), (FF // 64) ** -0.5, 0.625, ((0, 4), (1, 8)))
    cotangent = gaussian(key_list[10], (TOKENS, D), 1.0, 6.0, ((0, 32),))
    lengths = draw_lengths(jax.random.fold_in(key_list[13], 71), 0)
    deal = draw_deal(jax.random.fold_in(key_list[13], 71), 0)
    return dict(tokens=tokens, norm_attn=norm_attn, norm_ffn=norm_ffn, w_query=w_query, w_key=w_key, w_value=w_value, w_out=w_out, w_gate=w_gate, w_up=w_up, w_down=w_down, cotangent=cotangent, lengths=lengths, deal=deal)


@jax.custom_vjp
def low(v):
    return lax.optimization_barrier(v.astype(jnp.bfloat16)).astype(jnp.float32)

@jax.custom_vjp
def low_back(v):
    return v

def low_keep(v):
    return (low(v), None)

def low_pass(kept, grad):
    return (grad,)

def back_keep(v):
    return (v, None)

def back_low(kept, grad):
    return (low(grad),)
low.defvjp(low_keep, low_pass)
low_back.defvjp(back_keep, back_low)
BRANCH = 1.4 / math.sqrt(40.0)
EPSILON = 1e-05
NEGATIVE = -1e+30
PRECISE = lax.Precision.HIGHEST

def rotate(field_in, position, direction):
    head_count = field_in.shape[1] // HEAD_DIM
    half_dim = HEAD_DIM // 2
    counter = jnp.arange(half_dim, dtype=jnp.float32)
    frequency = jnp.exp(counter * (-2.0 * math.log(10000.0) / HEAD_DIM))
    phase_angle = position.astype(jnp.float32)[:, None] * frequency[None, :]
    cosine = jnp.concatenate([jnp.cos(phase_angle), jnp.cos(phase_angle)], axis=1)[:, None, :]
    sine_table = jnp.concatenate([jnp.sin(phase_angle), jnp.sin(phase_angle)], axis=1)[:, None, :]
    shaped = field_in.reshape(field_in.shape[0], head_count, HEAD_DIM)
    turned = jnp.concatenate([-shaped[:, :, half_dim:], shaped[:, :, :half_dim]], axis=2)
    return (shaped * cosine + direction * turned * sine_table).reshape(field_in.shape)

def matmul(left, right):
    return jnp.dot(left, right, precision=PRECISE)

def to_streams(flat_rows, deal):
    pieces = flat_rows.reshape(NBLK, BLK, D)[deal]
    shaped = pieces.reshape(N_WIDE, N_NARROW, MB, TOK_DEV // MB, D)
    return shaped.transpose(2, 0, 1, 3, 4).reshape(MB, N_WIDE * SLOT, D)

def from_streams(streams, deal):
    shaped = streams.reshape(MB, N_WIDE, N_NARROW, TOK_DEV // MB, D).transpose(1, 2, 0, 3, 4)
    pieces = shaped.reshape(NBLK, BLK, D)
    return jnp.zeros_like(pieces).at[deal].set(pieces).reshape(TOKENS, D)

def stream_layout(lengths):
    extent = (lengths + UNIT - 1) // UNIT * UNIT
    begin = jnp.cumsum(extent, axis=1) - extent
    places = jnp.arange(N_WIDE * SLOT, dtype=jnp.int32)
    ending = begin + lengths
    inside = (places[None, :, None] >= begin[:, None, :]) & (places[None, :, None] < ending[:, None, :])
    number = jnp.arange(N_WIDE, dtype=jnp.int32) + 1
    segment = (lax.optimization_barrier(jnp.sum(jnp.where(inside, number[None, None, :], 0), axis=2)) - 1).astype(jnp.int32)
    position = (places[None, :] - lax.optimization_barrier(jnp.sum(jnp.where(inside, begin[:, None, :], 0), axis=2))).astype(jnp.int32)
    return (segment, position)

def rank_attention(queries, keys, values, segment):
    query_three = queries.reshape(SLOT, HEADS, HEAD_DIM)
    key_three = keys.reshape(2 * SLOT, HEADS, HEAD_DIM)
    value_three = values.reshape(2 * SLOT, HEADS, HEAD_DIM)
    scores = jnp.einsum('qhd,khd->hqk', query_three, key_three, precision=PRECISE)
    scores = low_back(scores * (1.0 / math.sqrt(HEAD_DIM)))
    query_index = SLOT + jnp.arange(SLOT, dtype=jnp.int32)
    key_index = jnp.arange(2 * SLOT, dtype=jnp.int32)
    query_segment = segment[SLOT:]
    allowed = (query_segment[:, None] == segment[None, :]) & (query_segment[:, None] >= 0) & (key_index[None, :] <= query_index[:, None]) | (key_index[None, :] == query_index[:, None])
    scores = jnp.where(allowed[None, :, :], scores, NEGATIVE)
    top_score = lax.optimization_barrier(jnp.max(scores, axis=2, keepdims=True))
    weights_exp = jnp.exp(scores - top_score)
    probs = weights_exp / lax.optimization_barrier(jnp.sum(weights_exp, axis=2, keepdims=True))
    mixed = jnp.einsum('hqk,khd->qhd', low(probs), value_three, precision=PRECISE)
    return mixed.reshape(SLOT, HEADS * HEAD_DIM)

def step_rank(carry, parts):
    return (carry, jax.checkpoint(rank_attention)(*parts))

def with_previous(field_in, fill):
    shaped = field_in.reshape((N_WIDE, SLOT) + field_in.shape[1:])
    first = jnp.full((1, SLOT) + field_in.shape[1:], fill, field_in.dtype)
    earlier = jnp.concatenate([first, shaped[:-1]], axis=0)
    return jnp.concatenate([earlier, shaped], axis=1)

def layer(streams, gain_attn, gain_ffn, wq, wk, wv, wo, wg, wu, wd, validity, segment, position):
    results = []
    for micro in range(MB):
        resid = streams[micro] * validity[micro][:, None]
        rate_attn = lax.rsqrt(lax.optimization_barrier(jnp.mean(resid * resid, axis=1, keepdims=True)) + EPSILON)
        attn_in = low(resid * rate_attn * gain_attn[None, :])
        queries = low(rotate(low_back(matmul(attn_in, wq)), position[micro], 1.0))
        keys = low(rotate(low_back(matmul(attn_in, wk)), position[micro], 1.0))
        values = low(low_back(matmul(attn_in, wv)))
        carry_out, mixed = lax.scan(step_rank, jnp.zeros((), jnp.float32), (queries.reshape(N_WIDE, SLOT, D), with_previous(keys, 0.0), with_previous(values, 0.0), with_previous(segment[micro], -1)))
        attn_out = low(low_back(mixed.reshape(N_WIDE * SLOT, D)))
        branch_attn = low_back(matmul(attn_out, wo))
        middle = resid + BRANCH * branch_attn
        rate_ffn = lax.rsqrt(lax.optimization_barrier(jnp.mean(middle * middle, axis=1, keepdims=True)) + EPSILON)
        ffn_in = low(middle * rate_ffn * gain_ffn[None, :])
        gate = low_back(matmul(ffn_in, wg))
        upward = low_back(matmul(ffn_in, wu))
        hidden = low(jax.nn.silu(gate) * upward)
        branch_ffn = low_back(matmul(hidden, wd))
        results.append(middle + BRANCH * branch_ffn)
    return jnp.stack(results)

def reference(tokens, norm_attn, norm_ffn, w_query, w_key, w_value, w_out, w_gate, w_up, w_down, cotangent, lengths, deal):
    segment, position = stream_layout(lengths)
    validity = (segment >= 0).astype(jnp.float32)
    streams = to_streams(tokens, deal).astype(jnp.float32)
    cot_streams = to_streams(cotangent, deal).astype(jnp.float32)
    params = tuple((weight_arg.astype(jnp.float32) for weight_arg in (norm_attn, norm_ffn, w_query, w_key, w_value, w_out, w_gate, w_up, w_down)))

    def forward(streams_in, *weights_in):
        return layer(streams_in, *weights_in, validity, segment, position)
    result, pullback = jax.vjp(forward, streams, *params)
    grads = pullback(cot_streams)
    output = from_streams(result.astype(jnp.bfloat16), deal)
    grad_tokens = from_streams(grads[0].astype(jnp.bfloat16), deal)
    return (output, grad_tokens, grads[1], grads[2], grads[3], grads[4], grads[5], grads[6], grads[7], grads[8], grads[9])
```

```python
import math

import jax
import jax.numpy as jnp
from jax import lax
from jax.experimental import pallas as pl
from jax.experimental.pallas import tpu as pltpu
from jax.sharding import PartitionSpec as P

HEAD_DIM = 64
MB = 2
BLK = 8
UNIT = 64


BRANCH = 1.4 / math.sqrt(40.0)
EPSILON = 1e-05
NEGATIVE = -1e30
RING_MAX = 8


def ring_rank(place, count):
    place = lax.rem(place + 2 * count, count)
    return jnp.where(place < count // 2, 2 * place, 2 * count - 1 - 2 * place)


def ring_place(rank, count):
    return jnp.where(rank % 2 == 0, rank // 2, count - 1 - rank // 2)


def ring_send(block, count, direction):
    order = list(range(0, count, 2)) + list(range(count - 1, 0, -2))
    route = [(order[i], order[(i + direction) % count]) for i in range(count)]
    return lax.ppermute(block, "wide", route)


def after(value, *others):
    return lax.optimization_barrier((value,) + others)[0]


def ring_gather(block, count, gate=None):
    rank = lax.axis_index("wide")
    place = ring_place(rank, count)
    rows = block.shape[0]
    half = rows // 16 * 8
    found = [(rank, 0, block)]
    if gate is not None:
        block = after(block, *gate)
    up = down = block
    for step in range(1, count // 2):
        up = ring_send(up, count, 1)
        down = ring_send(down, count, -1)
        found.append((ring_rank(place - step, count), 0, up))
        found.append((ring_rank(place + step, count), 0, down))
    last = (up, down)
    far = ring_rank(place + count // 2, count)
    found.append((far, 0, ring_send(up[:half], count, 1)))
    found.append((far, half, ring_send(down[half:], count, -1)))
    return found, last


def assemble(found, count, rows, first=0):
    width = found[0][2].shape[1]
    full = jnp.zeros((count * rows, width), found[0][2].dtype)
    for rank, start, piece in found:
        low = max(first - start, 0)
        high = min(first + rows - start, piece.shape[0])
        if low < high:
            full = lax.dynamic_update_slice(
                full, piece[low:high], (rank * rows + start + low - first, 0)
            )
    return full


def gather_weights(groups, count):
    if count > RING_MAX:
        return [lax.all_gather(one, "wide", axis=0, tiled=True) for group in groups for one in group]
    fulls = []
    gate = None
    for group in groups:
        rows = group[0].shape[0]
        block = jnp.concatenate(group, axis=0) if len(group) > 1 else group[0]
        found, gate = ring_gather(block, count, gate)
        fulls += [assemble(found, count, rows, index * rows) for index in range(len(group))]
    return fulls


def ring_scatter(fulls, count):
    if count > RING_MAX:
        return [
            lax.psum_scatter(full, "wide", scatter_dimension=0, tiled=True).astype(jnp.float32)
            for full in fulls
        ]
    rank = lax.axis_index("wide")
    place = ring_place(rank, count)
    rows = fulls[0].shape[0] // count
    total = rows * len(fulls)
    half = total // 16 * 8

    def local(where):
        owner = ring_rank(where, count)
        return jnp.concatenate(
            [lax.dynamic_slice_in_dim(full, owner * rows, rows, axis=0) for full in fulls], axis=0
        ).astype(jnp.float32)

    far = local(place + count // 2).astype(jnp.bfloat16)
    up = ring_send(far[:half], count, 1)
    down = ring_send(far[half:], count, -1)
    for step in range(2, count // 2 + 1):
        mine_up = local(place + count // 2 - step + 1)
        mine_down = local(place - count // 2 + step - 1)
        if step == 2:
            sum_up = jnp.concatenate([up.astype(jnp.float32) + mine_up[:half], mine_up[half:]], axis=0)
            sum_down = jnp.concatenate(
                [mine_down[:half], down.astype(jnp.float32) + mine_down[half:]], axis=0
            )
        else:
            sum_up = up.astype(jnp.float32) + mine_up
            sum_down = down.astype(jnp.float32) + mine_down
        up = ring_send(sum_up.astype(jnp.bfloat16), count, 1)
        down = ring_send(sum_down.astype(jnp.bfloat16), count, -1)
    done = local(place) + up.astype(jnp.float32) + down.astype(jnp.float32)
    return [done[i * rows : (i + 1) * rows] for i in range(len(fulls))]


def swap_chip(block):
    return lax.ppermute(block, "narrow", [(0, 2), (1, 3), (2, 0), (3, 1)])


def swap_core(block):
    return lax.ppermute(block, "narrow", [(0, 1), (1, 0), (2, 3), (3, 2)])


def narrow_gather(block):
    lane = lax.axis_index("narrow")
    chip = swap_chip(block)
    core = swap_core(block)
    both = swap_core(chip)
    full = jnp.zeros((4,) + block.shape, block.dtype)
    for piece, owner in ((block, lane), (core, lane ^ 1), (chip, lane ^ 2), (both, lane ^ 3)):
        full = lax.dynamic_update_slice(full, piece[None], (owner,) + (0,) * block.ndim)
    return full


def narrow_scatter(parts):
    lane = lax.axis_index("narrow")

    def pick(owner):
        return lax.dynamic_index_in_dim(parts, owner, 0, keepdims=False)

    far = swap_core(pick(lane ^ 3))
    near = swap_core(pick(lane ^ 1))
    across = swap_chip(
        (pick(lane ^ 2).astype(jnp.float32) + far.astype(jnp.float32)).astype(jnp.bfloat16)
    )
    return pick(lane).astype(jnp.float32) + near.astype(jnp.float32) + across.astype(jnp.float32)


def angles(position):
    lane = jnp.arange(2 * HEAD_DIM, dtype=jnp.int32) % HEAD_DIM
    counter = (lane % (HEAD_DIM // 2)).astype(jnp.float32)
    frequency = jnp.exp(counter * (-2.0 * math.log(10000.0) / HEAD_DIM))
    phase_angle = position.astype(jnp.float32)[:, None] * frequency[None, :]
    sign = jnp.where(lane < HEAD_DIM // 2, -1.0, 1.0)
    return jnp.cos(phase_angle), jnp.sin(phase_angle) * sign[None, :]


def turn(field_in, cosine, sine, direction):
    rows, width = field_in.shape
    parts = []
    for low in range(0, width, 2 * HEAD_DIM):
        size = min(2 * HEAD_DIM, width - low)
        piece = field_in[:, low : low + size]
        if size < 2 * HEAD_DIM:
            piece = jnp.concatenate([piece, piece], axis=1)
        lane = lax.broadcasted_iota(jnp.int32, piece.shape, 1)
        swapped = jnp.where(
            lane % HEAD_DIM < HEAD_DIM // 2,
            pltpu.roll(piece, 2 * HEAD_DIM - HEAD_DIM // 2, 1),
            pltpu.roll(piece, HEAD_DIM // 2, 1),
        )
        parts.append((piece * cosine + direction * (swapped * sine))[:, :size])
    return jnp.concatenate(parts, axis=1)


def contract_rows(left, right):
    return lax.dot_general(
        left, right, (((0,), (0,)), ((), ())), preferred_element_type=jnp.float32
    ).astype(jnp.bfloat16)


def times(left, right):
    return jnp.dot(left, right, preferred_element_type=jnp.float32)


def times_transpose(left, right):
    return lax.dot_general(
        left, right, (((1,), (1,)), ((), ())), preferred_element_type=jnp.float32
    )


def norm_rate(resid):
    return lax.rsqrt(jnp.mean(resid * resid, axis=1, keepdims=True) + EPSILON)


def norm_backward(grad_in, resid, rate, gain):
    scaled_grad = grad_in * gain[None, :]
    return rate * scaled_grad - resid * rate**3 * jnp.mean(
        scaled_grad * resid, axis=1, keepdims=True
    )


def invert_order(placing):
    counter = jnp.arange(placing.shape[0], dtype=jnp.int32)
    return jnp.sum(jnp.where(placing[None, :] == counter[:, None], counter[None, :], 0), axis=1)


def deal_routes(deal, my_rank, my_lane, rank_count, lane_count, block_count):
    per_pair = block_count // rank_count
    base_block = (my_rank * lane_count + my_lane) * block_count
    counter = jnp.arange(block_count, dtype=jnp.int32)
    every_block = jnp.arange(deal.shape[0], dtype=jnp.int32)
    owned = base_block + counter
    target = jnp.sum(jnp.where(deal[None, :] == owned[:, None], every_block[None, :], 0), axis=1)
    target_rank = target // (lane_count * block_count)
    target_slot = target % block_count
    earlier = (target_rank[None, :] == target_rank[:, None]) & (
        target_slot[None, :] < target_slot[:, None]
    )
    send_place = target_rank * per_pair + jnp.sum(earlier.astype(jnp.int32), axis=1)
    mine = lax.dynamic_slice_in_dim(deal, base_block, block_count)
    source_rank = mine // (lane_count * block_count)
    before = (source_rank[None, :] == source_rank[:, None]) & (counter[None, :] < counter[:, None])
    recv_place = source_rank * per_pair + jnp.sum(before.astype(jnp.int32), axis=1)
    return (send_place, recv_place)


def stream_layout(length_row, my_rank, slot_rows):
    extent = (length_row + UNIT - 1) // UNIT * UNIT
    begin = jnp.cumsum(extent) - extent
    places = my_rank * slot_rows - slot_rows + jnp.arange(2 * slot_rows, dtype=jnp.int32)
    ending = begin + length_row
    inside = (places[:, None] >= begin[None, :]) & (places[:, None] < ending[None, :])
    number = jnp.arange(length_row.shape[0], dtype=jnp.int32) + 1
    segment = jnp.sum(jnp.where(inside, number[None, :], 0), axis=1) - 1
    position = places - jnp.sum(jnp.where(inside, begin[None, :], 0), axis=1)
    return (segment, position)


VMEM_LIMIT = 60 * 1024 * 1024


def dot_nn(left, right):
    return jnp.dot(left, right, preferred_element_type=jnp.float32)


def dot_nt(left, right):
    return times_transpose(left, right)


def dot_tn(left, right):
    return lax.dot_general(
        left, right, (((0,), (0,)), ((), ())), preferred_element_type=jnp.float32
    )


def project_kernel(rows_ref, weight_ref, cos_ref, sin_ref, q_ref, k_ref, v_ref):
    width = q_ref.shape[1]
    z = dot_nn(rows_ref[...], weight_ref[...])
    turned = turn(z[:, : 2 * width], cos_ref[...], sin_ref[...], 1.0).astype(jnp.bfloat16)
    q_ref[...] = turned[:, :width]
    k_ref[...] = turned[:, width:]
    v_ref[...] = z[:, 2 * width :].astype(jnp.bfloat16)


def project(rows, weight, cosine, sine):
    count, depth = rows.shape
    width = weight.shape[1] // 3
    block = 256
    out = jax.ShapeDtypeStruct((count, width), jnp.bfloat16)
    row_spec = pl.BlockSpec((block, width), lambda i: (i, 0))
    angle_spec = pl.BlockSpec((block, 2 * HEAD_DIM), lambda i: (i, 0))
    return pl.pallas_call(
        project_kernel,
        out_shape=(out, out, out),
        grid=(count // block,),
        in_specs=[
            pl.BlockSpec((block, depth), lambda i: (i, 0)),
            pl.BlockSpec(weight.shape, lambda i: (0, 0), pipeline_mode=pl.Buffered(1)),
            angle_spec,
            angle_spec,
        ],
        out_specs=(row_spec, row_spec, row_spec),
        compiler_params=pltpu.CompilerParams(vmem_limit_bytes=VMEM_LIMIT),
        cost_estimate=pl.CostEstimate(
            flops=2 * count * depth * 3 * width,
            bytes_accessed=2 * (count * depth + 3 * depth * width + 3 * count * width),
            transcendentals=0,
        ),
        name="project",
    )(rows, weight, cosine, sine)


def fill_bias(seg_col_ref, seg_row_ref, bias_own, bias_prev):
    slot = bias_own.shape[0]
    query = seg_row_ref[...]
    key = lax.broadcasted_iota(jnp.int32, (slot, slot), 0)
    place = lax.broadcasted_iota(jnp.int32, (slot, slot), 1)
    own = seg_col_ref[slot:, :]
    allowed = (own == query) & (query >= 0) & (key <= place) | (key == place)
    bias_own[...] = jnp.where(allowed, 0.0, NEGATIVE)
    bias_prev[...] = jnp.where((seg_col_ref[:slot, :] == query) & (query >= 0), 0.0, NEGATIVE)


def over_pairs(width, body):
    pairs = width // (2 * HEAD_DIM)

    def step(index, carry):
        body(pl.multiple_of(index * 2 * HEAD_DIM, 2 * HEAD_DIM), index * 2, 2)
        return carry

    lax.fori_loop(0, pairs, step, 0)
    if width % (2 * HEAD_DIM):
        body(pairs * 2 * HEAD_DIM, pairs * 2, 1)


def head_mask(lanes, head, value):
    lane = lax.broadcasted_iota(jnp.int32, (1, lanes), 1)
    return jnp.where(lane // HEAD_DIM == head, value, 0.0).astype(jnp.bfloat16)


def flat(ref, low, lanes):
    value = ref[:, :, pl.ds(low, lanes)]
    return value.reshape(value.shape[0] * value.shape[1], lanes)


def attend_kernel(
    flag_ref, seg_col_ref, seg_row_ref, q_ref, k_ref, v_ref, kp_ref, vp_ref,
    o_ref, lse_ref, bias_own, bias_prev,
):
    fill_bias(seg_col_ref, seg_row_ref, bias_own, bias_prev)
    slot = bias_own.shape[0]
    part = slot // 2

    def pair(with_prev, low, head, heads):
        lanes = heads * HEAD_DIM
        q, k, v = (flat(ref, low, lanes) for ref in (q_ref, k_ref, v_ref))
        if with_prev:
            kp, vp = kp_ref[:, pl.ds(low, lanes)], vp_ref[:, pl.ds(low, lanes)]
        for half in range(2):
            first, keys = half * part, (half + 1) * part
            mixed = []
            for one in range(heads):
                qm = q[first : first + part] * head_mask(lanes, one, 1.0 / math.sqrt(HEAD_DIM))
                s = dot_nt(k[:keys], qm) + bias_own[:keys, first : first + part]
                top = jnp.max(s, axis=0, keepdims=True)
                if with_prev:
                    sp = dot_nt(kp, qm) + bias_prev[:, first : first + part]
                    top = jnp.maximum(top, jnp.max(sp, axis=0, keepdims=True))
                p = jnp.exp(s - top)
                total = jnp.sum(p, axis=0, keepdims=True)
                o = dot_tn(v[:keys], p.astype(jnp.bfloat16))
                if with_prev:
                    pp = jnp.exp(sp - top)
                    total = total + jnp.sum(pp, axis=0, keepdims=True)
                    o = o + dot_tn(vp, pp.astype(jnp.bfloat16))
                mixed.append(o[one * HEAD_DIM : (one + 1) * HEAD_DIM] / total)
                lse_ref[pl.ds(head + one, 1), first : first + part] = top + jnp.log(total)
            o = jnp.concatenate(mixed, axis=0).T
            quarter = o_ref.shape[1]
            o_ref[first // quarter : (first + part) // quarter, :, pl.ds(low, lanes)] = (
                o.astype(jnp.bfloat16).reshape(part // quarter, quarter, lanes)
            )

    width = q_ref.shape[2]
    shared = flag_ref[pl.program_id(0)] == 1

    @pl.when(shared)
    def _():
        over_pairs(width, lambda *args: pair(True, *args))

    @pl.when(jnp.logical_not(shared))
    def _():
        over_pairs(width, lambda *args: pair(False, *args))


def attention_specs(lanes, rows, width):
    block = pl.BlockSpec((lanes, None, rows, width), lambda u, flag: (0, u, 0, 0))
    slot = lanes * rows
    key_before = pl.BlockSpec((None, None, slot, width), lambda u, flag: (u, 0, 0, 0))
    value_before = pl.BlockSpec((None, None, slot, width), lambda u, flag: (u, 1, 0, 0))
    col = pl.BlockSpec((None, 2 * slot, 1), lambda u, flag: (u, 0, 0))
    row = pl.BlockSpec((None, 1, slot), lambda u, flag: (u, 0, 0))
    lse = pl.BlockSpec((None, 16, slot), lambda u, flag: (u, 0, 0))
    return block, key_before, value_before, col, row, lse


def attend(flags, seg_col, seg_row, q, k, v, before):
    lanes, micros, rows, width = q.shape
    slot = lanes * rows
    block, key_before, value_before, col, row, lse = attention_specs(lanes, rows, width)
    heads = width // HEAD_DIM
    return pl.pallas_call(
        attend_kernel,
        out_shape=(
            jax.ShapeDtypeStruct(q.shape, jnp.bfloat16),
            jax.ShapeDtypeStruct((micros, 16, slot), jnp.float32),
        ),
        grid_spec=pltpu.PrefetchScalarGridSpec(
            num_scalar_prefetch=1,
            grid=(micros,),
            in_specs=[col, row, block, block, block, key_before, value_before],
            out_specs=(block, lse),
            scratch_shapes=[
                pltpu.VMEM((slot, slot), jnp.float32),
                pltpu.VMEM((slot, slot), jnp.float32),
            ],
        ),
        compiler_params=pltpu.CompilerParams(vmem_limit_bytes=VMEM_LIMIT),
        cost_estimate=pl.CostEstimate(
            flops=4 * micros * heads * slot * slot * 256,
            bytes_accessed=12 * micros * slot * width,
            transcendentals=micros * heads * slot * slot,
        ),
        name="attend",
    )(flags, seg_col, seg_row, q, k, v, before, before)


def attend_back_kernel(
    flag_ref, seg_col_ref, seg_row_ref, q_ref, k_ref, v_ref, kp_ref, vp_ref, o_ref, do_ref, lse_ref,
    dq_ref, dk_ref, dv_ref, back_ref, bias_own, bias_prev,
):
    fill_bias(seg_col_ref, seg_row_ref, bias_own, bias_prev)
    slot = bias_own.shape[0]
    part = slot // 2
    quarter = q_ref.shape[1]
    scale = 1.0 / math.sqrt(HEAD_DIM)

    def pair(with_prev, low, head, heads):
        lanes = heads * HEAD_DIM
        q, k, v, o, do = (flat(ref, low, lanes) for ref in (q_ref, k_ref, v_ref, o_ref, do_ref))
        if with_prev:
            kp, vp = kp_ref[:, pl.ds(low, lanes)], vp_ref[:, pl.ds(low, lanes)]
        product = (do.astype(jnp.float32) * o.astype(jnp.float32)).T
        dk = [0.0, 0.0]
        dv = [0.0, 0.0]
        dkp = dvp = 0.0
        for half in range(2):
            first, keys = half * part, (half + 1) * part
            turned = []
            for one in range(heads):
                span = slice(one * HEAD_DIM, (one + 1) * HEAD_DIM)
                delta = jnp.sum(product[span, first : first + part], axis=0, keepdims=True)
                lse = lse_ref[pl.ds(head + one, 1), first : first + part]
                qm = q[first : first + part] * head_mask(lanes, one, scale)
                dm = do[first : first + part] * head_mask(lanes, one, 1.0)
                p = jnp.exp(dot_nt(k[:keys], qm) + bias_own[:keys, first : first + part] - lse)
                ds = (p * (dot_nt(v[:keys], dm) - delta)).astype(jnp.bfloat16)
                new_dv = dot_nn(p.astype(jnp.bfloat16), dm)
                new_dk = dot_nn(ds, qm)
                for index in range(half + 1):
                    rows = slice(index * part, (index + 1) * part)
                    dv[index] = dv[index] + new_dv[rows]
                    dk[index] = dk[index] + new_dk[rows]
                dq = dot_tn(k[:keys], ds)
                if with_prev:
                    p = jnp.exp(dot_nt(kp, qm) + bias_prev[:, first : first + part] - lse)
                    ds = (p * (dot_nt(vp, dm) - delta)).astype(jnp.bfloat16)
                    dvp = dvp + dot_nn(p.astype(jnp.bfloat16), dm)
                    dkp = dkp + dot_nn(ds, qm)
                    dq = dq + dot_tn(kp, ds)
                turned.append(dq[span])
            dq = jnp.concatenate(turned, axis=0).T * scale
            dq_ref[first // quarter : (first + part) // quarter, :, pl.ds(low, lanes)] = dq.reshape(
                part // quarter, quarter, lanes
            )
        for index in range(2):
            span = slice(index * part // quarter, (index + 1) * part // quarter)
            shape = (part // quarter, quarter, lanes)
            dk_ref[span, :, pl.ds(low, lanes)] = dk[index].reshape(shape)
            dv_ref[span, :, pl.ds(low, lanes)] = dv[index].reshape(shape)
        if with_prev:
            back_ref[0, :, pl.ds(low, lanes)] = dkp.astype(jnp.bfloat16)
            back_ref[1, :, pl.ds(low, lanes)] = dvp.astype(jnp.bfloat16)

    width = q_ref.shape[2]
    shared = flag_ref[pl.program_id(0)] == 1

    @pl.when(shared)
    def _():
        over_pairs(width, lambda *args: pair(True, *args))

    @pl.when(jnp.logical_not(shared))
    def _():
        over_pairs(width, lambda *args: pair(False, *args))
        back_ref[...] = jnp.zeros_like(back_ref)


def attend_back(flags, seg_col, seg_row, q, k, v, before, o, do, lse_in):
    lanes, micros, rows, width = q.shape
    slot = lanes * rows
    block, key_before, value_before, col, row, lse = attention_specs(lanes, rows, width)
    both = pl.BlockSpec((None, 2, slot, width), lambda u, flag: (u, 0, 0, 0))
    wide = jax.ShapeDtypeStruct(q.shape, jnp.float32)
    heads = width // HEAD_DIM
    return pl.pallas_call(
        attend_back_kernel,
        out_shape=(
            wide,
            wide,
            wide,
            jax.ShapeDtypeStruct((micros, 2, slot, width), jnp.bfloat16),
        ),
        grid_spec=pltpu.PrefetchScalarGridSpec(
            num_scalar_prefetch=1,
            grid=(micros,),
            in_specs=[col, row, block, block, block, key_before, value_before, block, block, lse],
            out_specs=(block, block, block, both),
            scratch_shapes=[
                pltpu.VMEM((slot, slot), jnp.float32),
                pltpu.VMEM((slot, slot), jnp.float32),
            ],
        ),
        compiler_params=pltpu.CompilerParams(vmem_limit_bytes=VMEM_LIMIT),
        cost_estimate=pl.CostEstimate(
            flops=10 * micros * heads * slot * slot * 256,
            bytes_accessed=30 * micros * slot * width,
            transcendentals=micros * heads * slot * slot,
        ),
        name="attend_back",
    )(flags, seg_col, seg_row, q, k, v, before, before, o, do, lse_in)


def join_kernel(dq_ref, dk_ref, dv_ref, back_ref, cos_ref, sin_ref, out_ref):
    width = dq_ref.shape[1]
    cosine, sine = cos_ref[...], sin_ref[...]
    dk = dk_ref[...] + back_ref[0].astype(jnp.float32)
    dv = dv_ref[...] + back_ref[1].astype(jnp.float32)
    out_ref[...] = jnp.concatenate(
        [turn(dq_ref[...], cosine, sine, -1.0), turn(dk, cosine, sine, -1.0), dv], axis=1
    ).astype(jnp.bfloat16)


def join_grads(dq, dk, dv, back, cosine, sine):
    lanes, micros, rows, width = dq.shape
    block = pl.BlockSpec((None, None, rows, width), lambda j, u: (j, u, 0, 0))
    both = pl.BlockSpec((None, 2, rows, width), lambda j, u: (u, 0, j, 0))
    angle = pl.BlockSpec((None, None, rows, 2 * HEAD_DIM), lambda j, u: (j, u, 0, 0))
    return pl.pallas_call(
        join_kernel,
        out_shape=jax.ShapeDtypeStruct((lanes, micros, rows, 3 * width), jnp.bfloat16),
        grid=(lanes, micros),
        in_specs=[block, block, block, both, angle, angle],
        out_specs=pl.BlockSpec((None, None, rows, 3 * width), lambda j, u: (j, u, 0, 0)),
        compiler_params=pltpu.CompilerParams(vmem_limit_bytes=VMEM_LIMIT),
        cost_estimate=pl.CostEstimate(
            flops=8 * lanes * micros * rows * width,
            bytes_accessed=22 * lanes * micros * rows * width,
            transcendentals=0,
        ),
        name="join_grads",
    )(dq, dk, dv, back, cosine, sine)


def pair_route(micro, count, direction):
    route = [(low, low + 1) for low in range(micro, count - 1, 2)]
    return [(b, a) for a, b in route] if direction < 0 else route


def body(
    tokens,
    norm_attn,
    norm_ffn,
    w_query,
    w_key,
    w_value,
    w_out,
    w_gate,
    w_up,
    w_down,
    cotangent,
    lengths,
    deal,
):
    rank_count = lax.axis_size("wide")
    lane_count = lax.axis_size("narrow")
    my_rank = lax.axis_index("wide")
    my_lane = lax.axis_index("narrow")
    row_count = tokens.shape[0]
    width = tokens.shape[1]
    block_count = row_count // BLK
    per_pair = block_count // rank_count
    micro_rows = row_count // MB
    slot_rows = lane_count * micro_rows
    all_rows = lane_count * row_count
    features = w_query.shape[1]
    shard = w_query.shape[0]
    send_place, recv_place = deal_routes(
        deal, my_rank, my_lane, rank_count, lane_count, block_count
    )
    send_order = invert_order(send_place)
    back_order = invert_order(recv_place)

    def exchange(flat_rows, order, placing):
        packed = flat_rows.reshape(block_count, BLK, width)[order].reshape(
            rank_count, per_pair * BLK, width
        )
        got = lax.all_to_all(packed, "wide", split_axis=0, concat_axis=0, tiled=True)
        return got.reshape(block_count, BLK, width)[placing].reshape(row_count, width)

    dealt_x = exchange(tokens, send_order, recv_place)
    dealt_cot = exchange(cotangent, send_order, recv_place)

    wqkv, wo, wg, wu, wd = gather_weights(
        [
            [jnp.concatenate([w_query, w_key, w_value], axis=1)],
            [w_out.T],
            [w_gate, w_up],
            [w_down.T],
        ],
        rank_count,
    )

    gain_attn = norm_attn.astype(jnp.float32)
    gain_ffn = norm_ffn.astype(jnp.float32)
    layouts = [stream_layout(lengths[micro], my_rank, slot_rows) for micro in range(MB)]
    segments = [one[0] for one in layouts]
    own_segment = jnp.concatenate(
        [
            lax.dynamic_slice_in_dim(segment, slot_rows + my_lane * micro_rows, micro_rows)
            for segment in segments
        ]
    )
    validity = (own_segment >= 0).astype(jnp.float32)[:, None]
    by_lane = (lane_count, MB, micro_rows)
    row_position = jnp.stack(
        [one[1][slot_rows:].reshape(lane_count, micro_rows) for one in layouts], axis=1
    ).reshape(all_rows)
    cosine, sine = angles(row_position)
    seg_col = jnp.stack(segments)[:, :, None]
    seg_row = jnp.stack(segments)[:, None, slot_rows:]
    parity = jnp.arange(MB, dtype=jnp.int32)
    flags = ((my_rank > 0) & ((my_rank + parity) % 2 == 1)).astype(jnp.int32)

    resid = dealt_x.astype(jnp.float32) * validity
    rate_attn = norm_rate(resid)
    attn_in = (resid * rate_attn * gain_attn[None, :]).astype(jnp.bfloat16)
    attn_rows = narrow_gather(attn_in).reshape(all_rows, width)
    cot_all = narrow_gather(dealt_cot).reshape(all_rows, width)
    queries, keys, values = (
        one.reshape(by_lane + (features,)) for one in project(attn_rows, wqkv, cosine, sine)
    )
    before = jnp.stack(
        [
            lax.ppermute(
                jnp.stack([keys[:, micro], values[:, micro]]).reshape(2, slot_rows, features),
                "wide",
                pair_route(micro, rank_count, 1),
            )
            for micro in range(MB)
        ]
    )
    mixed, log_total = attend(flags, seg_col, seg_row, queries, keys, values, before)
    attn_out = mixed.reshape(all_rows, features)
    branch_attn = narrow_scatter(
        times_transpose(attn_out, wo).astype(jnp.bfloat16).reshape(lane_count, row_count, width)
    )
    middle = resid + BRANCH * branch_attn
    rate_ffn = norm_rate(middle)
    ffn_in = (middle * rate_ffn * gain_ffn[None, :]).astype(jnp.bfloat16)
    ffn_rows = narrow_gather(ffn_in).reshape(all_rows, width)
    gate = times(ffn_rows, wg)
    upward = times(ffn_rows, wu)
    sigma = jax.nn.sigmoid(gate)
    hidden = (gate * sigma * upward).astype(jnp.bfloat16)
    cot_branch = (BRANCH * cot_all.astype(jnp.float32)).astype(jnp.bfloat16)
    grad_wd = contract_rows(cot_branch, hidden)
    (sum_wd,) = ring_scatter([grad_wd], rank_count)
    grad_hidden = times(cot_branch, wd)
    grad_gate = (grad_hidden * upward * sigma * (1.0 + gate * (1.0 - sigma))).astype(jnp.bfloat16)
    grad_upward = (grad_hidden * gate * sigma).astype(jnp.bfloat16)
    grad_ffn_in = narrow_scatter(
        (times_transpose(grad_gate, wg) + times_transpose(grad_upward, wu))
        .astype(jnp.bfloat16)
        .reshape(lane_count, row_count, width)
    )
    grad_wg = contract_rows(ffn_rows, grad_gate)
    grad_wu = contract_rows(ffn_rows, grad_upward)
    sum_wg, sum_wu = ring_scatter([grad_wg, grad_wu], rank_count)
    branch_ffn = narrow_scatter(
        times_transpose(hidden, wd).astype(jnp.bfloat16).reshape(lane_count, row_count, width)
    )
    output = exchange(
        (middle + BRANCH * branch_ffn).astype(jnp.bfloat16), back_order, send_place
    )
    gain_total_ffn = jnp.sum(grad_ffn_in * middle * rate_ffn, axis=0)
    grad_middle = dealt_cot.astype(jnp.float32) + norm_backward(
        grad_ffn_in, middle, rate_ffn, gain_ffn
    )
    grad_branch = narrow_gather((BRANCH * grad_middle).astype(jnp.bfloat16)).reshape(
        all_rows, width
    )
    grad_mixed = times(grad_branch, wo).astype(jnp.bfloat16)
    grad_wo = contract_rows(grad_branch, attn_out)
    (sum_wo,) = ring_scatter([grad_wo], rank_count)

    grad_q, grad_k, grad_v, shared = attend_back(
        flags, seg_col, seg_row, queries, keys, values, before, mixed,
        grad_mixed.reshape(by_lane + (features,)), log_total,
    )
    back = jnp.stack(
        [
            lax.ppermute(shared[micro], "wide", pair_route(micro, rank_count, -1))
            for micro in range(MB)
        ]
    )
    angle_shape = by_lane + (2 * HEAD_DIM,)
    grad_qkv = join_grads(
        grad_q, grad_k, grad_v, back, cosine.reshape(angle_shape), sine.reshape(angle_shape)
    ).reshape(all_rows, 3 * features)
    grad_wqkv = contract_rows(attn_rows, grad_qkv)
    (sum_wqkv,) = ring_scatter([grad_wqkv], rank_count)
    grad_attn_in = narrow_scatter(
        times_transpose(grad_qkv, wqkv).astype(jnp.bfloat16).reshape(lane_count, row_count, width)
    )
    gain_total_attn = jnp.sum(grad_attn_in * resid * rate_attn, axis=0)
    grad_resid = grad_middle + norm_backward(grad_attn_in, resid, rate_attn, gain_attn)
    grad_tokens = exchange(
        (validity * grad_resid).astype(jnp.bfloat16), back_order, send_place
    )
    gain_sum_attn, gain_sum_ffn = lax.psum((gain_total_attn, gain_total_ffn), ("wide", "narrow"))
    return (
        output,
        grad_tokens,
        gain_sum_attn,
        gain_sum_ffn,
        sum_wqkv[:, :features],
        sum_wqkv[:, features : 2 * features],
        sum_wqkv[:, 2 * features :],
        sum_wo.T,
        sum_wg,
        sum_wu,
        sum_wd.T,
    )


def solution(mesh):
    placed = (
        P(("wide", "narrow"), None),
        P(),
        P(),
        P("wide", "narrow"),
        P("wide", "narrow"),
        P("wide", "narrow"),
        P("narrow", "wide"),
        P("wide", "narrow"),
        P("wide", "narrow"),
        P("narrow", "wide"),
        P(("wide", "narrow"), None),
        P(),
        P(),
    )
    return jax.shard_map(
        body,
        mesh=mesh,
        in_specs=placed,
        out_specs=(
            P(("wide", "narrow"), None),
            P(("wide", "narrow"), None),
            P(),
            P(),
            P("wide", "narrow"),
            P("wide", "narrow"),
            P("wide", "narrow"),
            P("narrow", "wide"),
            P("wide", "narrow"),
            P("wide", "narrow"),
            P("narrow", "wide"),
        ),
        check_vma=False,
    )
```

```python
import math

import jax
import jax.numpy as jnp
from jax import lax
from jax.experimental import pallas as pl
from jax.experimental.layout import Layout, with_layout_constraint
from jax.experimental.pallas import tpu as pltpu
from jax.sharding import PartitionSpec as P

HEAD_DIM = 64
MB = 2
BLK = 8
UNIT = 64


BRANCH = 1.4 / math.sqrt(40.0)
EPSILON = 1e-05
NEGATIVE = -1e30
RING_MAX = 8
RING_MAX = 8


def ring_rank(place, count):
    place = lax.rem(place + 2 * count, count)
    return jnp.where(place < count // 2, 2 * place, 2 * count - 1 - 2 * place)


def ring_place(rank, count):
    return jnp.where(rank % 2 == 0, rank // 2, count - 1 - rank // 2)


def ring_send(block, count, direction):
    order = list(range(0, count, 2)) + list(range(count - 1, 0, -2))
    route = [(order[i], order[(i + direction) % count]) for i in range(count)]
    return lax.ppermute(block, "wide", route)


def after(value, *others):
    return lax.optimization_barrier((value,) + others)[0] if others else value


class Order:
    def __init__(self):
        self.marks = ()

    def tie(self, value):
        return after(value, *self.marks)

    def at(self, *marks):
        self.marks = tuple(marks)

    def land(self, *arrived):
        self.marks = self.marks + tuple(arrived)


PLAN = {'r1': 'wd', 'r2': 'split', 'r3': 'da2', 'r4': 'wu', 'e1': 'wu', 'e2': 'far3', 'e3': 'both3', 'e4': 'back2', 'u1': 'wqkv', 'u2': 'da1', 'u3': 'norm4', 'o1': '@q3', 'g1': '@o3', 'd1': '@g3', 'O': 'da1', 'P6': 1, 'W': 'wqkv', 'f1': 'wo', 'f2': 'da1', 'f3': 'norm4', 'f4': 'deal'}
LAND = {'r1': 'da2', 'r2': 'wg', 'r3': 'yf', 'r4': 'norm3', 'e1': 'norm3', 'e2': 'mixed', 'e3': 'back1', 'e4': 'da1', 'u1': 'sum4', 'u3': 'unpack', 'f1': 'sum4', 'f2': 'norm4', 'f3': 'unpack'}
MADE = {'e4': 'back1', 'e2': 'gather3'}


class Plan:
    def __init__(self, order):
        self.order, self.rings, self.sent = order, {}, {}
        self.passed = set()

    def add(self, name, ring):
        self.rings[name], self.sent[name] = ring, 0
        self.push(())

    def push(self, marks):
        for name, ring in self.rings.items():
            while self.sent[name] < ring.count // 2:
                step = PLAN.get(name + str(self.sent[name] + 1))
                if step is not None and step[0] == "@":
                    if self.sent.get(step[1], 0) < int(step[2]):
                        break
                    self.order.at(*self.hop(step[1:]))
                elif step is not None and step not in self.passed:
                    break
                else:
                    self.order.at(*(marks if step is not None else ()))
                ring.send(self.order)
                self.sent[name] += 1
        self.order.at()

    def hop(self, name):
        hops = self.rings[name[0]].hops
        return hops[int(name[1]) - 1] if hops else ()

    def done(self, step, *marks):
        self.passed.add(step)
        self.push(marks)

    def before(self, step, value):
        marks = []
        for name, ready in LAND.items():
            if ready == step and self.sent.get(name[0], 0) >= int(name[1]):
                marks += self.hop(name)
        for name, ready in MADE.items():
            if ready == step and self.sent.get(name[0], 0) >= int(name[1]):
                marks += self.rings[name[0]].messages[int(name[1]) - 1 :][:1] and list(
                    self.rings[name[0]].messages[int(name[1]) - 1]
                )
        return after(value, *marks)


class RingGather:
    def __init__(self, group, count):
        self.group, self.count, self.hops, self.messages = group, count, [], []
        self.block = jnp.concatenate(group, axis=0) if len(group) > 1 else group[0]

    def send(self, order):
        if self.count > RING_MAX:
            return
        up, down = self.hops[-1] if self.hops else (self.block, self.block)
        if len(self.hops) == self.count // 2 - 1:
            half = self.block.shape[0] // 16 * 8
            up, down = up[:half], down[half:]
            order.land(up, down)
        up, down = order.tie(up), order.tie(down)
        self.messages.append((up, down))
        self.hops.append((ring_send(up, self.count, 1), ring_send(down, self.count, -1)))

    def arrived(self):
        return self.hops[-1] if self.hops else ()

    def hop(self, index):
        return self.hops[index] if self.hops else ()

    def all(self, order):
        for _ in range(self.count // 2):
            self.send(order)
            order.at()

    def gathered(self):
        rows = self.group[0].shape[0]
        if not self.hops:
            fulls = [lax.all_gather(one, "wide", axis=0, tiled=True) for one in self.group]
            return [([full], [(0, 0, full.shape[0], None, 0)], rows) for full in fulls]
        far = self.count // 2
        found = []
        for step, (up, down) in enumerate(self.hops[:-1], 1):
            found += [(-step, 0, up), (step, 0, down)]
        up, down = self.hops[-1]
        found += [(far, 0, up), (far, up.shape[0], down)]
        out = []
        for index, own in enumerate(self.group):
            arrays, moves = [own], [(0, 0, rows, 0, 0)]
            first = index * rows
            for shift, start, piece in found:
                low = max(first, start)
                high = min(first + rows, start + piece.shape[0])
                if low < high:
                    arrays.append(piece)
                    moves.append((len(arrays) - 1, low - start, high - low, shift, low - first))
            out.append((arrays, moves, rows))
        return out


class RingSum:
    def __init__(self, fulls, count, where):
        self.fulls, self.count, self.where = fulls, count, where
        self.rows = fulls[0].shape[0] // count
        self.last = ()
        self.hops, self.messages = [], []
        self.hop = 0
        self.place = ring_place(lax.axis_index("wide"), count)
        self.half = self.rows * len(fulls) // 16 * 8

    def arrived(self):
        return self.last

    def local(self, shift):
        owner = ring_rank(self.place + shift, self.count)
        return jnp.concatenate(
            [
                lax.dynamic_slice_in_dim(full, owner * self.rows, self.rows, axis=0)
                for full in self.fulls
            ],
            axis=0,
        )

    def send(self, order):
        if self.count > RING_MAX:
            return
        self.hop += 1
        far, half = self.count // 2, self.half
        if self.hop == 1:
            both = self.local(far)
            up, down = order.tie(both[:half]), order.tie(both[half:])
        else:
            up, down = ring_add(
                self.where, self.count, far - self.hop + 1, self.fulls,
                order.tie(self.last[0]), self.last[1],
            )
        self.messages.append((up, down))
        self.last = (ring_send(up, self.count, 1), ring_send(down, self.count, -1))
        self.hops.append(self.last)

    def finish(self):
        if self.count > RING_MAX:
            return [
                lax.psum_scatter(full, "wide", scatter_dimension=0, tiled=True).astype(jnp.float32)
                for full in self.fulls
            ]
        up, down = self.last
        done = (
            self.local(0).astype(jnp.float32) + up.astype(jnp.float32) + down.astype(jnp.float32)
        )
        return [done[i * self.rows : (i + 1) * self.rows] for i in range(len(self.fulls))]


def swap_chip(block):
    return lax.ppermute(block, "narrow", [(0, 2), (1, 3), (2, 0), (3, 1)])


def swap_core(block):
    return lax.ppermute(block, "narrow", [(0, 1), (1, 0), (2, 3), (3, 2)])


class LaneGather:
    def __init__(self, block, order):
        self.block = order.tie(block)
        self.chip = swap_chip(self.block)
        self.core = swap_core(self.block)

    def finish(self, order):
        self.pieces = [self.block, self.core, self.chip, swap_core(order.tie(self.chip))]
        return self.pieces

    def whole(self):
        lane = lax.axis_index("narrow")
        full = jnp.zeros((4,) + self.block.shape, self.block.dtype)
        for index, piece in enumerate(self.pieces):
            full = lax.dynamic_update_slice(
                full, piece[None], (lane ^ index,) + (0,) * self.block.ndim
            )
        return full


class LaneSum:
    def __init__(self, own, across, pair, order):
        self.own, self.across = own, across
        self.got = swap_core(order.tie(pair))

    def cross(self, order):
        both = self.across.astype(jnp.float32) + self.got[0].astype(jnp.float32)
        both = order.tie(both.astype(jnp.bfloat16))
        order.land(both)
        self.far = swap_chip(both)

    def finish(self):
        return (
            self.own.astype(jnp.float32)
            + self.got[1].astype(jnp.float32)
            + self.far.astype(jnp.float32)
        )


def sum_over(value, axis, count):
    step = 1
    while step < count:
        value = value + lax.ppermute(value, axis, [(i, i ^ step) for i in range(count)])
        step *= 2
    return value


def angles(position):
    lane = jnp.arange(2 * HEAD_DIM, dtype=jnp.int32) % HEAD_DIM
    counter = (lane % (HEAD_DIM // 2)).astype(jnp.float32)
    frequency = jnp.exp(counter * (-2.0 * math.log(10000.0) / HEAD_DIM))
    phase_angle = position.astype(jnp.float32)[:, None] * frequency[None, :]
    sign = jnp.where(lane < HEAD_DIM // 2, -1.0, 1.0)
    return jnp.cos(phase_angle), jnp.sin(phase_angle) * sign[None, :]


def turn(field_in, cosine, sine, direction):
    rows, width = field_in.shape
    parts = []
    for low in range(0, width, 2 * HEAD_DIM):
        size = min(2 * HEAD_DIM, width - low)
        piece = field_in[:, low : low + size]
        if size < 2 * HEAD_DIM:
            piece = jnp.concatenate([piece, piece], axis=1)
        lane = lax.broadcasted_iota(jnp.int32, piece.shape, 1)
        swapped = jnp.where(
            lane % HEAD_DIM < HEAD_DIM // 2,
            pltpu.roll(piece, 2 * HEAD_DIM - HEAD_DIM // 2, 1),
            pltpu.roll(piece, HEAD_DIM // 2, 1),
        )
        parts.append((piece * cosine + direction * (swapped * sine))[:, :size])
    return jnp.concatenate(parts, axis=1)


def row_major(value):
    return with_layout_constraint(value, Layout(major_to_minor=tuple(range(value.ndim))))


def contract_rows(left, right):
    product = lax.dot_general(
        left, right, (((0,), (0,)), ((), ())), preferred_element_type=jnp.float32
    )
    return row_major(product.astype(jnp.bfloat16))


def times(left, right):
    return jnp.dot(left, right, preferred_element_type=jnp.float32)


def times_transpose(left, right):
    return lax.dot_general(
        left, right, (((1,), (1,)), ((), ())), preferred_element_type=jnp.float32
    )


def norm_rate(resid):
    return lax.rsqrt(jnp.mean(resid * resid, axis=1, keepdims=True) + EPSILON)


def norm_backward(grad_in, resid, rate, gain):
    scaled_grad = grad_in * gain[None, :]
    return rate * scaled_grad - resid * rate**3 * jnp.mean(
        scaled_grad * resid, axis=1, keepdims=True
    )


def invert_order(placing):
    counter = jnp.arange(placing.shape[0], dtype=jnp.int32)
    return jnp.sum(jnp.where(placing[None, :] == counter[:, None], counter[None, :], 0), axis=1)


def deal_routes(deal, my_rank, my_lane, rank_count, lane_count, block_count):
    per_pair = block_count // rank_count
    base_block = (my_rank * lane_count + my_lane) * block_count
    counter = jnp.arange(block_count, dtype=jnp.int32)
    every_block = jnp.arange(deal.shape[0], dtype=jnp.int32)
    owned = base_block + counter
    target = jnp.sum(jnp.where(deal[None, :] == owned[:, None], every_block[None, :], 0), axis=1)
    target_rank = target // (lane_count * block_count)
    target_slot = target % block_count
    earlier = (target_rank[None, :] == target_rank[:, None]) & (
        target_slot[None, :] < target_slot[:, None]
    )
    send_place = target_rank * per_pair + jnp.sum(earlier.astype(jnp.int32), axis=1)
    mine = lax.dynamic_slice_in_dim(deal, base_block, block_count)
    source_rank = mine // (lane_count * block_count)
    before = (source_rank[None, :] == source_rank[:, None]) & (counter[None, :] < counter[:, None])
    recv_place = source_rank * per_pair + jnp.sum(before.astype(jnp.int32), axis=1)
    return (send_place, recv_place)


def stream_layout(length_row, my_rank, slot_rows):
    extent = (length_row + UNIT - 1) // UNIT * UNIT
    begin = jnp.cumsum(extent) - extent
    places = my_rank * slot_rows - slot_rows + jnp.arange(2 * slot_rows, dtype=jnp.int32)
    ending = begin + length_row
    inside = (places[:, None] >= begin[None, :]) & (places[:, None] < ending[None, :])
    number = jnp.arange(length_row.shape[0], dtype=jnp.int32) + 1
    segment = jnp.sum(jnp.where(inside, number[None, :], 0), axis=1) - 1
    position = places - jnp.sum(jnp.where(inside, begin[None, :], 0), axis=1)
    return (segment, position)


VMEM_LIMIT = 60 * 1024 * 1024


def dot_nn(left, right):
    return jnp.dot(left, right, preferred_element_type=jnp.float32)


def dot_nt(left, right):
    return times_transpose(left, right)


def dot_tn(left, right):
    return lax.dot_general(
        left, right, (((0,), (0,)), ((), ())), preferred_element_type=jnp.float32
    )


def params():
    return pltpu.CompilerParams(vmem_limit_bytes=VMEM_LIMIT)


def cost(flops, bytes_accessed, transcendentals=0):
    return pl.CostEstimate(
        flops=flops, bytes_accessed=bytes_accessed, transcendentals=transcendentals
    )


ANY = pl.BlockSpec(memory_space=pl.ANY)


class Collector:
    def __init__(self, gathered):
        self.arrays, self.moves, self.rows = gathered
        self.height = self.rows * lax.axis_size("wide")
        self.width = self.arrays[0].shape[1]
        self.shape = jax.ShapeDtypeStruct((self.height, self.width), jnp.bfloat16)

    def scratch(self):
        return [
            pltpu.VMEM((self.height, self.width), jnp.bfloat16),
            pltpu.SemaphoreType.DMA((len(self.moves) + 1,)),
        ]

    def copies(self, where, refs, whole, sems):
        count = self.height // self.rows
        for index, (array, start, rows, shift, offset) in enumerate(self.moves):
            row = offset
            if shift is not None:
                owner = ring_rank(ring_place(where[2], count) + shift, count)
                row = pl.multiple_of(owner * self.rows + offset, 16)
            yield pltpu.make_async_copy(
                refs[array].at[pl.ds(start, rows), :], whole.at[pl.ds(row, rows), :], sems.at[index]
            )

    def start(self, *args):
        for copy in self.copies(*args):
            copy.start()

    def wait(self, *args):
        for copy in self.copies(*args):
            copy.wait()

    def out(self, whole, out_ref, sems):
        return pltpu.make_async_copy(whole, out_ref, sems.at[len(self.moves)])


class Lanes:
    def __init__(self, pieces):
        self.pieces = list(pieces)
        self.block = pieces[0].shape
        self.shape = jax.ShapeDtypeStruct((4,) + self.block, jnp.bfloat16)

    def scratch(self):
        return [pltpu.VMEM((4,) + self.block, jnp.bfloat16), pltpu.SemaphoreType.DMA((4,))]

    def start(self, refs, rows, sems):
        for index in range(4):
            pltpu.make_async_copy(refs[index], rows.at[index], sems.at[index]).start()

    def wait(self, step, refs, rows, sems):
        pltpu.make_async_copy(refs[0], rows.at[step], sems.at[step]).wait()


def by_lane(rows, width):
    return pl.BlockSpec((None, rows, width), lambda i, where: (where[0] ^ i, 0, 0))


def fixed(*shape):
    return pl.BlockSpec(shape, lambda i, where: (0,) * len(shape))


def whole(*shape):
    return pl.BlockSpec(
        shape, lambda i, where: (0,) * len(shape), pipeline_mode=pl.Buffered(1)
    )


def by_parity(parity, both):
    half = both.shape[0] // 2
    low, high = both[:half], both[half:]
    return jnp.where(parity == 0, low, high), jnp.where(parity == 0, high, low)


def project_kernel(weight, lanes, where, *refs):
    count = len(weight.arrays)
    weights, refs = refs[:count], refs[count:]
    pieces, refs = refs[:4], refs[4:]
    cos_ref, sin_ref, q_ref, send_ref, keep_ref, w_out, rows_out, w, w_sems, rows, r_sems, o_sems = refs
    skip = weight.width - 3 * q_ref.shape[-1]
    step = pl.program_id(0)

    @pl.when(step == 0)
    def _():
        lanes.start(pieces, rows, r_sems)
        weight.start(where, weights, w, w_sems)
        weight.wait(where, weights, w, w_sems)
        weight.out(w, w_out, w_sems).start()

    lanes.wait(step, pieces, rows, r_sems)
    pltpu.make_async_copy(rows.at[step], rows_out.at[where[0] ^ step], o_sems.at[step]).start()
    width = q_ref.shape[-1]
    z = dot_nn(rows[step], w[:, skip:])
    turned = turn(z[:, : 2 * width], cos_ref[...], sin_ref[...], 1.0)
    first, second = by_parity(where[1], turned[:, :width])
    q_ref[0], q_ref[1] = first.astype(jnp.bfloat16), second.astype(jnp.bfloat16)
    first, second = by_parity(where[1], pack_pair(turned[:, width:], z[:, 2 * width :]))
    send_ref[...], keep_ref[...] = first.astype(jnp.bfloat16), second.astype(jnp.bfloat16)

    @pl.when(step == 3)
    def _():
        weight.out(w, w_out, w_sems).wait()
        for index in range(4):
            pltpu.make_async_copy(rows.at[index], rows_out.at[index], o_sems.at[index]).wait()


def project(where, gathered, width, pieces, cosine, sine):
    weight, lanes = Collector(gathered), Lanes(pieces)
    count, depth = lanes.block
    angle = by_lane(count, 2 * HEAD_DIM)
    pair = pl.BlockSpec((2, None, count // 2, width), lambda i, where: (0, where[0] ^ i, 0, 0))
    out = jax.ShapeDtypeStruct((2, 4, count // 2, width), jnp.bfloat16)
    both = jax.ShapeDtypeStruct((4, count // 2, 2 * width), jnp.bfloat16)
    both_spec = by_lane(count // 2, 2 * width)
    return pl.pallas_call(
        lambda *refs: project_kernel(weight, lanes, *refs),
        out_shape=(out, both, both, weight.shape, lanes.shape),
        grid_spec=pltpu.PrefetchScalarGridSpec(
            num_scalar_prefetch=1,
            grid=(4,),
            in_specs=[ANY] * (len(weight.arrays) + 4) + [angle, angle],
            out_specs=(pair, both_spec, both_spec, ANY, ANY),
            scratch_shapes=weight.scratch() + lanes.scratch() + [pltpu.SemaphoreType.DMA((4,))],
        ),
        compiler_params=params(),
        cost_estimate=cost(8 * count * depth * 3 * width, 40 * count * depth),
        name="project",
    )(where, *weight.arrays, *lanes.pieces, cosine, sine)


def put_relative(step, value, own_ref, across_ref, pair_ref):
    @pl.when(step == 0)
    def _():
        own_ref[...] = value

    @pl.when(step == 2)
    def _():
        across_ref[...] = value

    @pl.when(step == 3)
    def _():
        pair_ref[0] = value

    @pl.when(step == 1)
    def _():
        pair_ref[1] = value


def relative_out(rows, width):
    shapes = (
        jax.ShapeDtypeStruct((rows, width), jnp.bfloat16),
        jax.ShapeDtypeStruct((rows, width), jnp.bfloat16),
        jax.ShapeDtypeStruct((2, rows, width), jnp.bfloat16),
    )
    specs = (whole(rows, width), whole(rows, width), whole(2, rows, width))
    return shapes, specs


def part_of(weight, width):
    columns = width if weight.shape[1] == width else (width + 127) // 128 * 128
    return pl.BlockSpec(
        (weight.shape[0], columns), lambda i, where: (0, 0), pipeline_mode=pl.Buffered(1)
    )


def merge_kernel(weight, where, *refs):
    count = len(weight.arrays)
    weights, refs = refs[:count], refs[count:]
    a_ref, b_ref, own_ref, across_ref, pair_ref, o_ref, w_out, w, w_sems = refs
    step = pl.program_id(0)

    @pl.when(step == 0)
    def _():
        weight.start(where, weights, w, w_sems)
        weight.wait(where, weights, w, w_sems)
        weight.out(w, w_out, w_sems).start()

    low, high = by_parity(where[1], jnp.concatenate([a_ref[...], b_ref[...]], axis=0))
    rows = jnp.concatenate([low, high], axis=0)
    o_ref[...] = rows
    put_relative(step, dot_nt(rows, w[...]).astype(jnp.bfloat16), own_ref, across_ref, pair_ref)

    @pl.when(step == 3)
    def _():
        weight.out(w, w_out, w_sems).wait()


def merge(where, gathered, first, second):
    weight = Collector(gathered)
    lanes, rows, width = first.shape
    shapes, specs = relative_out(2 * rows, weight.height)
    return pl.pallas_call(
        lambda *refs: merge_kernel(weight, *refs),
        out_shape=shapes + (jax.ShapeDtypeStruct((lanes, 2 * rows, width), jnp.bfloat16), weight.shape),
        grid_spec=pltpu.PrefetchScalarGridSpec(
            num_scalar_prefetch=1,
            grid=(4,),
            in_specs=[ANY] * len(weight.arrays) + [by_lane(rows, width)] * 2,
            out_specs=specs + (by_lane(2 * rows, width), ANY),
            scratch_shapes=weight.scratch(),
        ),
        compiler_params=params(),
        cost_estimate=cost(16 * rows * width * weight.height, 20 * rows * weight.height),
        name="merge",
    )(where, *weight.arrays, first, second)


def hidden_kernel(gate_w, up_w, lanes, where, *refs):
    gates, refs = refs[: len(gate_w.arrays)], refs[len(gate_w.arrays) :]
    ups, refs = refs[: len(up_w.arrays)], refs[len(up_w.arrays) :]
    pieces, refs = refs[:4], refs[4:]
    gate_ref, up_ref, hidden_ref, g_out, u_out, rows_out, g, g_sems, u, u_sems, rows, r_sems, o_sems = refs
    step = pl.program_id(0)

    @pl.when(step == 0)
    def _():
        lanes.start(pieces, rows, r_sems)
        gate_w.start(where, gates, g, g_sems)
        up_w.start(where, ups, u, u_sems)
        gate_w.wait(where, gates, g, g_sems)
        gate_w.out(g, g_out, g_sems).start()

    lanes.wait(step, pieces, rows, r_sems)
    pltpu.make_async_copy(rows.at[step], rows_out.at[where[0] ^ step], o_sems.at[step]).start()
    gate = dot_nn(rows[step], g[...])
    gate_ref[...] = gate

    @pl.when(step == 0)
    def _():
        up_w.wait(where, ups, u, u_sems)
        up_w.out(u, u_out, u_sems).start()

    up = dot_nn(rows[step], u[...])
    up_ref[...] = up
    hidden_ref[...] = (gate * jax.nn.sigmoid(gate) * up).astype(jnp.bfloat16)

    @pl.when(step == 3)
    def _():
        gate_w.out(g, g_out, g_sems).wait()
        up_w.out(u, u_out, u_sems).wait()
        for index in range(4):
            pltpu.make_async_copy(rows.at[index], rows_out.at[index], o_sems.at[index]).wait()


def hidden_units(where, gathered_gate, gathered_up, pieces):
    gate_w, up_w, lanes = Collector(gathered_gate), Collector(gathered_up), Lanes(pieces)
    rows, depth = lanes.block
    width = gate_w.width
    wide = jax.ShapeDtypeStruct((4, rows, width), jnp.float32)
    return pl.pallas_call(
        lambda *refs: hidden_kernel(gate_w, up_w, lanes, *refs),
        out_shape=(
            wide, wide, jax.ShapeDtypeStruct((4, rows, width), jnp.bfloat16),
            gate_w.shape, up_w.shape, lanes.shape,
        ),
        grid_spec=pltpu.PrefetchScalarGridSpec(
            num_scalar_prefetch=1,
            grid=(4,),
            in_specs=[ANY] * (len(gate_w.arrays) + len(up_w.arrays) + 4),
            out_specs=(by_lane(rows, width),) * 3 + (ANY,) * 3,
            scratch_shapes=gate_w.scratch() + up_w.scratch() + lanes.scratch()
            + [pltpu.SemaphoreType.DMA((4,))],
        ),
        compiler_params=params(),
        cost_estimate=cost(16 * rows * depth * width, 60 * rows * width, 4 * rows * width),
        name="hidden_units",
    )(where, *gate_w.arrays, *up_w.arrays, *lanes.pieces)


def split_kernel(down_w, where, *refs):
    downs, refs = refs[: len(down_w.arrays)], refs[len(down_w.arrays) :]
    cot_ref, gate_ref, up_ref, dg_ref, du_ref, d_out, d, d_sems = refs
    step = pl.program_id(0)

    @pl.when(step == 0)
    def _():
        down_w.start(where, downs, d, d_sems)
        down_w.wait(where, downs, d, d_sems)
        down_w.out(d, d_out, d_sems).start()

    grad = dot_nn(cot_ref[...], d[...])
    gate, up = gate_ref[...], up_ref[...]
    sigma = jax.nn.sigmoid(gate)
    part = grad * sigma
    dg_ref[...] = (part * up * (1.0 + gate * (1.0 - sigma))).astype(jnp.bfloat16)
    du_ref[...] = (part * gate).astype(jnp.bfloat16)

    @pl.when(step == 3)
    def _():
        down_w.out(d, d_out, d_sems).wait()


def split_grads(where, gathered, cot, gate, up):
    down_w = Collector(gathered)
    lanes, rows, width = gate.shape
    depth = cot.shape[2]
    narrow = jax.ShapeDtypeStruct(gate.shape, jnp.bfloat16)
    block = by_lane(rows, width)
    return pl.pallas_call(
        lambda *refs: split_kernel(down_w, *refs),
        out_shape=(narrow, narrow, down_w.shape),
        grid_spec=pltpu.PrefetchScalarGridSpec(
            num_scalar_prefetch=1,
            grid=(4,),
            in_specs=[ANY] * len(down_w.arrays) + [by_lane(rows, depth), block, block],
            out_specs=(block, block, ANY),
            scratch_shapes=down_w.scratch(),
        ),
        compiler_params=params(),
        cost_estimate=cost(8 * rows * depth * width, 60 * rows * width, 4 * rows * width),
        name="split_grads",
    )(where, *down_w.arrays, cot, gate, up)


def terms_kernel(count, where, *refs):
    total = None
    for index in range(count):
        rows, weight = refs[index][...], refs[count + index]
        term = dot_nt(rows, weight[:, weight.shape[1] - rows.shape[1] :])
        total = term if total is None else total + term
    put_relative(pl.program_id(0), total.astype(jnp.bfloat16), *refs[2 * count :])


def terms(where, pairs):
    rows = pairs[0][0].shape[1]
    height = pairs[0][1].shape[0]
    shapes, specs = relative_out(rows, height)
    depth = sum(weight.shape[1] for _, weight in pairs)
    return pl.pallas_call(
        lambda *refs: terms_kernel(len(pairs), *refs),
        out_shape=shapes,
        grid_spec=pltpu.PrefetchScalarGridSpec(
            num_scalar_prefetch=1,
            grid=(4,),
            in_specs=[by_lane(rows, one.shape[2]) for one, _ in pairs]
            + [whole(*weight.shape) for _, weight in pairs],
            out_specs=specs,
        ),
        compiler_params=params(),
        cost_estimate=cost(8 * rows * height * depth, 2 * (4 * rows + height) * depth),
        name="terms",
    )(where, *[one for one, _ in pairs], *[weight for _, weight in pairs])


def mixed_kernel(lanes, where, *refs):
    pieces, refs = refs[:4], refs[4:]
    w_ref, out_ref, rows_out, rows, r_sems, o_sems = refs
    step = pl.program_id(0)

    @pl.when(step == 0)
    def _():
        lanes.start(pieces, rows, r_sems)

    lanes.wait(step, pieces, rows, r_sems)
    pltpu.make_async_copy(rows.at[step], rows_out.at[where[0] ^ step], o_sems.at[step]).start()
    out = dot_nn(rows[step], w_ref[:, : out_ref.shape[-1]])
    first, second = by_parity(where[1], out)
    out_ref[0], out_ref[1] = first.astype(jnp.bfloat16), second.astype(jnp.bfloat16)

    @pl.when(step == 3)
    def _():
        for index in range(4):
            pltpu.make_async_copy(rows.at[index], rows_out.at[index], o_sems.at[index]).wait()


def mixed_grads(where, weight, width, pieces):
    lanes = Lanes(pieces)
    count, depth = lanes.block
    return pl.pallas_call(
        lambda *refs: mixed_kernel(lanes, *refs),
        out_shape=(jax.ShapeDtypeStruct((2, 4, count // 2, width), jnp.bfloat16), lanes.shape),
        grid_spec=pltpu.PrefetchScalarGridSpec(
            num_scalar_prefetch=1,
            grid=(4,),
            in_specs=[ANY] * 4 + [part_of(weight, width)],
            out_specs=(
                pl.BlockSpec((2, None, count // 2, width), lambda i, where: (0, where[0] ^ i, 0, 0)),
                ANY,
            ),
            scratch_shapes=lanes.scratch() + [pltpu.SemaphoreType.DMA((4,))],
        ),
        compiler_params=params(),
        cost_estimate=cost(8 * count * depth * width, 20 * count * depth),
        name="mixed_grads",
    )(where, *lanes.pieces, weight)


def ring_add_kernel(count, split, where, *refs):
    ups, downs, refs = refs[:count], refs[count : 2 * count], refs[2 * count :]
    up_in, down_in, up_out, down_out = refs
    step = pl.program_id(0)
    for index in range(count):

        @pl.when(step // 2 == index)
        def _():
            up = ups[index][...].astype(jnp.float32)
            down = downs[index][...].astype(jnp.float32)
            if split:
                up = jnp.where(step < count, up + up_in[...].astype(jnp.float32), up)
                down = jnp.where(step < count, down, down + down_in[...].astype(jnp.float32))
            else:
                up = up + up_in[...].astype(jnp.float32)
                down = down + down_in[...].astype(jnp.float32)
            up_out[...] = up.astype(jnp.bfloat16)
            down_out[...] = down.astype(jnp.bfloat16)


def ring_add(where, ranks, shift, fulls, up, down):
    count = len(fulls)
    rows, width = fulls[0].shape[0] // ranks, fulls[0].shape[1]
    part = rows // 2
    split = up.shape[0] < rows * count

    def local(index, direction):
        def at(i, where):
            owner = ring_rank(ring_place(where[2], ranks) + direction * shift, ranks)
            return (owner * 2 + jnp.clip(i - 2 * index, 0, 1), 0)

        return pl.BlockSpec((part, width), at)

    block = pl.BlockSpec((part, width), lambda i, where: (i, 0))
    upper, lower = block, block
    if split:
        upper = pl.BlockSpec((part, width), lambda i, where: (jnp.minimum(i, count - 1), 0))
        lower = pl.BlockSpec((part, width), lambda i, where: (jnp.maximum(i - count, 0), 0))
    out = jax.ShapeDtypeStruct((rows * count, width), jnp.bfloat16)
    return pl.pallas_call(
        lambda *refs: ring_add_kernel(count, split, *refs),
        out_shape=(out, out),
        grid_spec=pltpu.PrefetchScalarGridSpec(
            num_scalar_prefetch=1,
            grid=(2 * count,),
            in_specs=[local(index, 1) for index in range(count)]
            + [local(index, -1) for index in range(count)]
            + [upper, lower],
            out_specs=(block, block),
        ),
        compiler_params=params(),
        cost_estimate=cost(4 * rows * count * width, 12 * rows * count * width),
        name="ring_add",
    )(where, *fulls, *fulls, up, down)


def fill_bias(seg_col_ref, seg_row_ref, bias_own, bias_prev):
    slot = bias_own.shape[0]
    query = seg_row_ref[...]
    key = lax.broadcasted_iota(jnp.int32, (slot, slot), 0)
    place = lax.broadcasted_iota(jnp.int32, (slot, slot), 1)
    own = seg_col_ref[slot:, :]
    allowed = (own == query) & (query >= 0) & (key <= place) | (key == place)
    bias_own[...] = jnp.where(allowed, 0.0, NEGATIVE)
    if bias_prev is not None:
        before = seg_col_ref[:slot, :]
        bias_prev[...] = jnp.where((before == query) & (query >= 0), 0.0, NEGATIVE)


def over_pairs(width, body):
    pairs = width // (2 * HEAD_DIM)

    def step(index, carry):
        body(pl.multiple_of(index * 2 * HEAD_DIM, 2 * HEAD_DIM), index * 2, 2)
        return carry

    lax.fori_loop(0, pairs, step, 0)
    if width % (2 * HEAD_DIM):
        body(pairs * 2 * HEAD_DIM, pairs * 2, 1)


def head_mask(lanes, head, value):
    lane = lax.broadcasted_iota(jnp.int32, (1, lanes), 1)
    return jnp.where(lane // HEAD_DIM == head, value, 0.0).astype(jnp.bfloat16)


def flat(ref, low, lanes):
    value = ref[:, :, pl.ds(low, lanes)]
    return value.reshape(value.shape[0] * value.shape[1], lanes)


def pack_pair(keys, values):
    even = keys.shape[1] // (2 * HEAD_DIM) * 2 * HEAD_DIM
    return jnp.concatenate(
        [keys[:, :even], values[:, :even], keys[:, even:], values[:, even:]], axis=1
    )


def split_pair(both):
    width = both.shape[1] // 2
    even = width // (2 * HEAD_DIM) * 2 * HEAD_DIM
    odd = width - even
    return (
        jnp.concatenate([both[:, :even], both[:, 2 * even : 2 * even + odd]], axis=1),
        jnp.concatenate([both[:, even : 2 * even], both[:, 2 * even + odd :]], axis=1),
    )


def pair_lane(low, heads, which, width):
    even = width // (2 * HEAD_DIM) * 2 * HEAD_DIM
    if heads == 2:
        return pl.multiple_of(low + which * even, 2 * HEAD_DIM)
    return 2 * even + which * HEAD_DIM


def attend_kernel(with_prev, seg_col_ref, seg_row_ref, q_ref, kv_ref, *refs):
    if with_prev:
        before_ref, o_ref, lse_ref, bias_own, bias_prev = refs
    else:
        o_ref, lse_ref, bias_own = refs
        bias_prev = None
    fill_bias(seg_col_ref, seg_row_ref, bias_own, bias_prev)
    slot = bias_own.shape[0]
    part = slot // 2

    def pair(low, head, heads):
        lanes = heads * HEAD_DIM
        q = flat(q_ref, low, lanes)
        at_k, at_v = (pair_lane(low, heads, which, q_ref.shape[2]) for which in range(2))
        k, v = flat(kv_ref, at_k, lanes), flat(kv_ref, at_v, lanes)
        if with_prev:
            kp, vp = flat(before_ref, at_k, lanes), flat(before_ref, at_v, lanes)
        for half in range(2):
            first, keys = half * part, (half + 1) * part
            mixed = []
            for one in range(heads):
                qm = q[first : first + part] * head_mask(lanes, one, 1.0 / math.sqrt(HEAD_DIM))
                s = dot_nt(k[:keys], qm) + bias_own[:keys, first : first + part]
                top = jnp.max(s, axis=0, keepdims=True)
                if with_prev:
                    sp = dot_nt(kp, qm) + bias_prev[:, first : first + part]
                    top = jnp.maximum(top, jnp.max(sp, axis=0, keepdims=True))
                p = jnp.exp(s - top)
                total = jnp.sum(p, axis=0, keepdims=True)
                o = dot_tn(v[:keys], p.astype(jnp.bfloat16))
                if with_prev:
                    pp = jnp.exp(sp - top)
                    total = total + jnp.sum(pp, axis=0, keepdims=True)
                    o = o + dot_tn(vp, pp.astype(jnp.bfloat16))
                mixed.append(o[one * HEAD_DIM : (one + 1) * HEAD_DIM] / total)
                lse_ref[pl.ds(head + one, 1), first : first + part] = top + jnp.log(total)
            o = jnp.concatenate(mixed, axis=0).T
            quarter = o_ref.shape[1]
            o_ref[first // quarter : (first + part) // quarter, :, pl.ds(low, lanes)] = (
                o.astype(jnp.bfloat16).reshape(part // quarter, quarter, lanes)
            )

    over_pairs(q_ref.shape[2], pair)


def attend(slot, seg_col, seg_row, q, kv, before=None):
    _, lanes, rows, width = q.shape
    count = lanes * rows
    heads = width // HEAD_DIM
    with_prev = before is not None
    both = pl.BlockSpec((lanes, rows, 2 * width), lambda i: (0, 0, 0))
    return pl.pallas_call(
        lambda *refs: attend_kernel(with_prev, *refs),
        out_shape=(
            jax.ShapeDtypeStruct((lanes, rows, width), jnp.bfloat16),
            jax.ShapeDtypeStruct((16, count), jnp.float32),
        ),
        grid=(1,),
        in_specs=slot_specs(slot, lanes, rows, width) + [both] * (2 if with_prev else 1),
        out_specs=(
            pl.BlockSpec((lanes, rows, width), lambda i: (0, 0, 0)),
            pl.BlockSpec((16, count), lambda i: (0, 0)),
        ),
        scratch_shapes=[pltpu.VMEM((count, count), jnp.float32)] * (2 if with_prev else 1),
        compiler_params=params(),
        cost_estimate=cost(
            (5 if with_prev else 2) * heads * count * count * 256,
            12 * count * width,
            heads * count * count,
        ),
        name="attend",
    )(seg_col, seg_row, q, kv, *([before] if with_prev else []))


def slot_specs(slot, lanes, rows, width):
    count = lanes * rows
    return [
        pl.BlockSpec((None, 2 * count, 1), lambda i: (slot, 0, 0)),
        pl.BlockSpec((None, 1, count), lambda i: (slot, 0, 0)),
        pl.BlockSpec((None, lanes, rows, width), lambda i: (slot, 0, 0, 0)),
    ]


def attend_back_kernel(
    with_prev, seg_col_ref, seg_row_ref, q_ref, kv_ref, o_ref, do_ref, lse_ref, *refs
):
    if with_prev:
        before_ref, dq_ref, dk_ref, dv_ref, back_ref, bias_own, bias_prev = refs
    else:
        dq_ref, dk_ref, dv_ref, bias_own = refs
        bias_prev = None
    fill_bias(seg_col_ref, seg_row_ref, bias_own, bias_prev)
    slot = bias_own.shape[0]
    part = slot // 2
    quarter = q_ref.shape[1]
    scale = 1.0 / math.sqrt(HEAD_DIM)

    def pair(low, head, heads):
        lanes = heads * HEAD_DIM
        q, o, do = (flat(ref, low, lanes) for ref in (q_ref, o_ref, do_ref))
        at_k, at_v = (pair_lane(low, heads, which, q_ref.shape[2]) for which in range(2))
        k, v = flat(kv_ref, at_k, lanes), flat(kv_ref, at_v, lanes)
        if with_prev:
            kp, vp = flat(before_ref, at_k, lanes), flat(before_ref, at_v, lanes)
        product = (do.astype(jnp.float32) * o.astype(jnp.float32)).T
        dk = [0.0, 0.0]
        dv = [0.0, 0.0]
        dkp = dvp = 0.0
        for half in range(2):
            first, keys = half * part, (half + 1) * part
            turned = []
            for one in range(heads):
                span = slice(one * HEAD_DIM, (one + 1) * HEAD_DIM)
                delta = jnp.sum(product[span, first : first + part], axis=0, keepdims=True)
                lse = lse_ref[pl.ds(head + one, 1), first : first + part]
                qm = q[first : first + part] * head_mask(lanes, one, scale)
                dm = do[first : first + part] * head_mask(lanes, one, 1.0)
                p = jnp.exp(dot_nt(k[:keys], qm) + bias_own[:keys, first : first + part] - lse)
                ds = (p * (dot_nt(v[:keys], dm) - delta)).astype(jnp.bfloat16)
                new_dv = dot_nn(p.astype(jnp.bfloat16), dm)
                new_dk = dot_nn(ds, qm)
                for index in range(half + 1):
                    rows = slice(index * part, (index + 1) * part)
                    dv[index] = dv[index] + new_dv[rows]
                    dk[index] = dk[index] + new_dk[rows]
                dq = dot_tn(k[:keys], ds)
                if with_prev:
                    p = jnp.exp(dot_nt(kp, qm) + bias_prev[:, first : first + part] - lse)
                    ds = (p * (dot_nt(vp, dm) - delta)).astype(jnp.bfloat16)
                    dvp = dvp + dot_nn(p.astype(jnp.bfloat16), dm)
                    dkp = dkp + dot_nn(ds, qm)
                    dq = dq + dot_tn(kp, ds)
                turned.append(dq[span])
            dq = jnp.concatenate(turned, axis=0).T * scale
            dq_ref[first // quarter : (first + part) // quarter, :, pl.ds(low, lanes)] = dq.reshape(
                part // quarter, quarter, lanes
            )
        for index in range(2):
            span = slice(index * part // quarter, (index + 1) * part // quarter)
            shape = (part // quarter, quarter, lanes)
            dk_ref[span, :, pl.ds(low, lanes)] = dk[index].reshape(shape)
            dv_ref[span, :, pl.ds(low, lanes)] = dv[index].reshape(shape)
        if with_prev:
            shape = (slot // quarter, quarter, lanes)
            back_ref[:, :, pl.ds(at_k, lanes)] = dkp.astype(jnp.bfloat16).reshape(shape)
            back_ref[:, :, pl.ds(at_v, lanes)] = dvp.astype(jnp.bfloat16).reshape(shape)

    over_pairs(q_ref.shape[2], pair)


def attend_back(slot, seg_col, seg_row, q, kv, o, do, lse_in, before=None):
    _, lanes, rows, width = q.shape
    count = lanes * rows
    heads = width // HEAD_DIM
    with_prev = before is not None
    both = pl.BlockSpec((lanes, rows, 2 * width), lambda i: (0, 0, 0))
    one = pl.BlockSpec((lanes, rows, width), lambda i: (0, 0, 0))
    specs = slot_specs(slot, lanes, rows, width)
    wide = jax.ShapeDtypeStruct((lanes, rows, width), jnp.float32)
    sent = jax.ShapeDtypeStruct((lanes, rows, 2 * width), jnp.bfloat16)
    return pl.pallas_call(
        lambda *refs: attend_back_kernel(with_prev, *refs),
        out_shape=(wide, wide, wide) + ((sent,) if with_prev else ()),
        grid=(1,),
        in_specs=specs
        + [both, one, specs[2], pl.BlockSpec((16, count), lambda i: (0, 0))]
        + ([both] if with_prev else []),
        out_specs=(one, one, one) + ((both,) if with_prev else ()),
        scratch_shapes=[pltpu.VMEM((count, count), jnp.float32)] * (2 if with_prev else 1),
        compiler_params=params(),
        cost_estimate=cost(
            (12 if with_prev else 5) * heads * count * count * 256,
            30 * count * width,
            heads * count * count,
        ),
        name="attend_back",
    )(seg_col, seg_row, q, kv, o, do, lse_in, *([before] if with_prev else []))


def join_kernel(where, *refs):
    dq_a, dk_a, dv_a, dq_b, dk_b, dv_b, back_ref, cos_ref, sin_ref, out_ref = refs
    cos_a, cos_b = by_parity(where[1], cos_ref[...])
    sin_a, sin_b = by_parity(where[1], sin_ref[...])
    dk_back, dv_back = split_pair(back_ref[...])
    dk = dk_a[...] + dk_back.astype(jnp.float32)
    dv = dv_a[...] + dv_back.astype(jnp.float32)
    first = jnp.concatenate(
        [turn(dq_a[...], cos_a, sin_a, -1.0), turn(dk, cos_a, sin_a, -1.0), dv], axis=1
    )
    second = jnp.concatenate(
        [turn(dq_b[...], cos_b, sin_b, -1.0), turn(dk_b[...], cos_b, sin_b, -1.0), dv_b[...]], axis=1
    )
    half = first.shape[0]
    out_ref[:half] = jnp.where(where[1] == 0, first, second).astype(jnp.bfloat16)
    out_ref[half:] = jnp.where(where[1] == 0, second, first).astype(jnp.bfloat16)


def join_grads(where, first, second, back, cosine, sine):
    lanes, rows, width = first[0].shape
    block = by_lane(rows, width)
    both = by_lane(rows, 2 * width)
    angle = by_lane(2 * rows, 2 * HEAD_DIM)
    return pl.pallas_call(
        join_kernel,
        out_shape=jax.ShapeDtypeStruct((lanes, 2 * rows, 3 * width), jnp.bfloat16),
        grid_spec=pltpu.PrefetchScalarGridSpec(
            num_scalar_prefetch=1,
            grid=(lanes,),
            in_specs=[block] * 6 + [both, angle, angle],
            out_specs=by_lane(2 * rows, 3 * width),
        ),
        compiler_params=params(),
        cost_estimate=cost(16 * lanes * rows * width, 44 * lanes * rows * width),
        name="join_grads",
    )(where, *first, *second, back, cosine, sine)


def to_next(block, count, direction):
    route = [(low, low + 1) for low in range(count - 1)]
    return lax.ppermute(block, "wide", [(b, a) for a, b in route] if direction < 0 else route)


def body(
    tokens,
    norm_attn,
    norm_ffn,
    w_query,
    w_key,
    w_value,
    w_out,
    w_gate,
    w_up,
    w_down,
    cotangent,
    lengths,
    deal,
):
    rank_count = lax.axis_size("wide")
    lane_count = lax.axis_size("narrow")
    my_rank = lax.axis_index("wide")
    my_lane = lax.axis_index("narrow")
    row_count = tokens.shape[0]
    width = tokens.shape[1]
    block_count = row_count // BLK
    per_pair = block_count // rank_count
    micro_rows = row_count // MB
    slot_rows = lane_count * micro_rows
    all_rows = lane_count * row_count
    features = w_query.shape[1]
    shard = w_query.shape[0]
    send_place, recv_place = deal_routes(
        deal, my_rank, my_lane, rank_count, lane_count, block_count
    )
    send_order = invert_order(send_place)
    back_order = invert_order(recv_place)

    def exchange(flat_rows, order_of, extra=None):
        packed = flat_rows.reshape(block_count, BLK, width)[order_of].reshape(
            rank_count, per_pair * BLK, width
        )
        if extra is not None:
            extra = jnp.broadcast_to(extra[None], (rank_count,) + extra.shape)
            packed = jnp.concatenate([packed, extra], axis=1)
        return lax.all_to_all(order.tie(packed), "wide", split_axis=0, concat_axis=0, tiled=True)

    def unpack(got, placing):
        rows = got[:, : per_pair * BLK]
        return rows.reshape(block_count, BLK, width)[placing].reshape(row_count, width)

    def rows_of(array):
        return array.reshape(all_rows, array.shape[-1])

    order = Order()
    plan = Plan(order)
    ring_qkv = RingGather([jnp.concatenate([w_query, w_key, w_value], axis=1)], rank_count)
    ring_out = RingGather([w_out.T], rank_count)
    ring_ffn = RingGather([w_gate, w_up], rank_count)
    ring_down = RingGather([w_down.T], rank_count)
    for name, ring in (("q", ring_qkv), ("o", ring_out), ("g", ring_ffn), ("d", ring_down)):
        plan.add(name, ring)

    got_x = exchange(tokens, send_order)
    plan.done("start")
    if "C" not in PLAN:
        got_cot = exchange(cotangent, send_order)

    gain_attn = norm_attn.astype(jnp.float32)
    gain_ffn = norm_ffn.astype(jnp.float32)
    parity = my_rank % 2
    where = jnp.stack([my_lane, parity, my_rank]).astype(jnp.int32)
    layouts = [stream_layout(lengths[micro], my_rank, slot_rows) for micro in range(MB)]
    own_segment = jnp.concatenate(
        [
            lax.dynamic_slice_in_dim(one[0], slot_rows + my_lane * micro_rows, micro_rows)
            for one in layouts
        ]
    )
    validity = (own_segment >= 0).astype(jnp.float32)[:, None]
    row_position = jnp.stack(
        [one[1][slot_rows:].reshape(lane_count, micro_rows) for one in layouts], axis=1
    ).reshape(all_rows)
    cosine, sine = (
        one.reshape(lane_count, row_count, 2 * HEAD_DIM) for one in angles(row_position)
    )
    segments = [one[0] for one in layouts]
    by_slot = jnp.where(parity == 0, jnp.stack(segments), jnp.stack(segments[::-1]))
    seg_col = by_slot[:, :, None]
    seg_row = by_slot[:, None, slot_rows:]

    dealt_x = unpack(got_x, recv_place)
    resid = dealt_x.astype(jnp.float32) * validity
    rate_attn = norm_rate(resid)
    attn_in = (resid * rate_attn * gain_attn[None, :]).astype(jnp.bfloat16)
    attn_in = plan.before("norm1", attn_in)
    rows_attn = LaneGather(attn_in, order).finish(order)
    plan.done("norm1", attn_in)
    (got_qkv,) = ring_qkv.gathered()
    rows_attn[0] = plan.before("project", rows_attn[0])
    queries, sent_kv, kept_kv, wqkv, attn_rows = project(
        where, got_qkv, features, rows_attn, cosine, sine
    )
    before = to_next(sent_kv, rank_count, 1)
    plan.done("project", queries)
    out_first, lse_first = attend(
        0, seg_col, seg_row, plan.before("attend1", queries), sent_kv
    )
    plan.done("attend1", out_first)
    if PLAN.get("C") == "attend1":
        got_cot = exchange(after(cotangent, out_first), send_order)
    out_second, lse_second = attend(
        1, seg_col, seg_row, queries, plan.before("attend2", after(kept_kv, out_first)), before
    )
    plan.done("attend2", out_second)
    (got_out,) = ring_out.gathered()
    own, across, pair, attn_out, w_out_full = merge(
        where, got_out, out_first, plan.before("merge", out_second)
    )
    plan.done("merge", pair)
    if PLAN.get("C") == "merge":
        got_cot = exchange(after(cotangent, pair), send_order)
    sum_attn = LaneSum(own, across, pair, order)
    sum_attn.got = plan.before("cross1", sum_attn.got)
    sum_attn.cross(order)
    plan.done("cross1", sum_attn.got)
    if PLAN.get("C") == "cross1":
        got_cot = exchange(after(cotangent, sum_attn.got), send_order)
    order.at()
    middle = resid + BRANCH * sum_attn.finish()
    rate_ffn = norm_rate(middle)
    ffn_in = (middle * rate_ffn * gain_ffn[None, :]).astype(jnp.bfloat16)
    ffn_in = plan.before("norm2", ffn_in)
    gather_ffn = LaneGather(ffn_in, order)
    plan.done("norm2", ffn_in)
    gather_ffn.chip = plan.before("both2", gather_ffn.chip)
    rows_ffn = gather_ffn.finish(order)
    plan.done("both2", gather_ffn.chip)
    dealt_cot = unpack(got_cot, recv_place)
    cot_in = (BRANCH * dealt_cot.astype(jnp.float32)).astype(jnp.bfloat16)
    if PLAN.get("X"):
        cot_in = after(cot_in, {"norm2": ffn_in, "both2": gather_ffn.chip, "merge": pair}[PLAN["X"]])
    gather_cot = LaneGather(cot_in, order)
    gather_cot.finish(order)
    cot_branch = gather_cot.whole()
    (got_gate, got_up) = ring_ffn.gathered()
    rows_ffn[0] = plan.before("hidden", rows_ffn[0])
    gate, upward, hidden, wg, wu, ffn_rows = hidden_units(
        where, got_gate, got_up, rows_ffn
    )
    plan.done("hidden", hidden)
    grad_wd = contract_rows(rows_of(cot_branch), rows_of(plan.before("wd", hidden)))
    plan.add("r", RingSum([grad_wd], rank_count, where))
    plan.done("wd", grad_wd)
    (got_down,) = ring_down.gathered()
    grad_gate, grad_upward, wd = split_grads(
        where, got_down, plan.before("split", after(cot_branch, grad_wd)), gate, upward
    )
    plan.done("split", grad_gate)
    own, across, pair = terms(
        where, [(plan.before("da2", grad_gate), wg), (grad_upward, wu)]
    )
    plan.done("da2", pair)
    sum_grad_ffn = LaneSum(own, across, pair, order)
    grad_wg = contract_rows(
        rows_of(ffn_rows), rows_of(plan.before("wg", after(grad_gate, pair)))
    )
    plan.done("wg", grad_wg)
    sum_grad_ffn.got = plan.before("cross2", after(sum_grad_ffn.got, grad_wg))
    sum_grad_ffn.cross(order)
    order.at()
    grad_wu = contract_rows(
        rows_of(ffn_rows),
        rows_of(plan.before("wu", after(grad_upward, grad_wg, sum_grad_ffn.got))),
    )
    plan.add("e", RingSum([grad_wg, grad_wu], rank_count, where))
    plan.done("wu", grad_wu)
    own, across, pair = terms(where, [(plan.before("yf", after(hidden, grad_wu)), wd)])
    plan.done("yf", pair)
    sum_grad_ffn.far = plan.before("norm3", after(sum_grad_ffn.far, pair))
    plan.done("far3", sum_grad_ffn.far)
    grad_ffn_in = sum_grad_ffn.finish()
    grad_middle = dealt_cot.astype(jnp.float32) + norm_backward(
        grad_ffn_in, middle, rate_ffn, gain_ffn
    )
    grad_branch_in = (BRANCH * grad_middle).astype(jnp.bfloat16)
    gather_branch = LaneGather(plan.before("gather3", grad_branch_in), order)
    plan.done("norm3", gather_branch.block)
    gain_total_ffn = jnp.sum(grad_ffn_in * middle * rate_ffn, axis=0)
    sum_down_out = LaneSum(own, across, after(pair, gather_branch.block), order)
    gather_branch.chip = plan.before("both3", after(gather_branch.chip, sum_down_out.got))
    rows_branch = gather_branch.finish(order)
    plan.done("both3", gather_branch.chip)
    order.at(gather_branch.chip)
    sum_down_out.cross(order)
    order.at()
    rows_branch[0] = plan.before("mixed", rows_branch[0])
    grad_mixed, grad_branch = mixed_grads(where, w_out_full, features, rows_branch)
    plan.done("mixed", grad_mixed)
    late = PLAN.get("W", "wqkv")
    if late == "mixed":
        grad_wo = contract_rows(rows_of(grad_branch), rows_of(after(attn_out, grad_mixed)))
        plan.add("f", RingSum([grad_wo], rank_count, where))
        plan.done("wo", grad_wo)
        grad_mixed = after(grad_mixed, grad_wo)
    *grads_second, shared = attend_back(
        1, seg_col, seg_row, queries, kept_kv, out_second,
        plan.before("back2", grad_mixed), lse_second, before
    )
    back = to_next(shared, rank_count, -1)
    plan.done("back2", shared)
    grads_first = attend_back(
        0, seg_col, seg_row, queries, sent_kv, out_first,
        plan.before(
            "back1", after(grad_mixed, shared, *((sum_down_out.far,) if PLAN.get("P6") else ()))
        ),
        lse_first
    )
    plan.done("back1", grads_first[0])
    if late == "back1":
        grad_wo = contract_rows(rows_of(grad_branch), rows_of(after(attn_out, grads_first[0])))
        plan.add("f", RingSum([grad_wo], rank_count, where))
        plan.done("wo", grad_wo)
        back = after(back, grad_wo)
    output_rows = (middle + BRANCH * sum_down_out.finish()).astype(jnp.bfloat16)
    ready = PLAN.get("O")
    if ready in ("back1", "back2"):
        output_rows = after(output_rows, grads_first[0] if ready == "back1" else shared)
        got_output = exchange(output_rows, back_order)
    grad_qkv = join_grads(
        where, grads_first, grads_second,
        plan.before("join", after(back, grads_first[0])), cosine, sine
    )
    plan.done("join", grad_qkv)
    grad_wqkv = contract_rows(rows_of(attn_rows), rows_of(plan.before("wqkv", grad_qkv)))
    plan.add("u", RingSum([grad_wqkv], rank_count, where))
    plan.done("wqkv", grad_wqkv)
    tail = grad_wqkv
    if late == "wqkv":
        grad_wo = contract_rows(rows_of(grad_branch), rows_of(after(attn_out, grad_wqkv)))
        plan.add("f", RingSum([grad_wo], rank_count, where))
        plan.done("wo", grad_wo)
        tail = grad_wo
    if ready not in ("back1", "back2", "da1"):
        got_output = exchange(after(output_rows, tail), back_order)
    own, across, pair = terms(
        where,
        [
            (
                plan.before(
                    "da1", after(grad_qkv, tail, *((got_output,) if PLAN.get("OL") == "da1" else ()))
                ),
                wqkv,
            )
        ],
    )
    if ready == "da1":
        got_output = exchange(after(output_rows, pair), back_order)
    pair = plan.before("sum4", pair)
    if PLAN.get("OL") == "sum4":
        pair = after(pair, got_output)
    plan.done("da1", pair)
    sum_grad_attn = LaneSum(own, across, pair, order)
    sum_grad_attn.got = plan.before("cross4", sum_grad_attn.got)
    sum_grad_attn.cross(order)
    plan.done("cross4", sum_grad_attn.got)
    sum_grad_attn.far = plan.before("norm4", sum_grad_attn.far)
    grad_attn_in = sum_grad_attn.finish()
    gain_total_attn = jnp.sum(grad_attn_in * resid * rate_attn, axis=0)
    grad_resid = grad_middle + norm_backward(grad_attn_in, resid, rate_attn, gain_attn)
    gains = jnp.stack([gain_total_attn, gain_total_ffn])
    main = gains.astype(jnp.bfloat16)
    rest = (gains - main.astype(jnp.float32)).astype(jnp.bfloat16)
    extra = jnp.concatenate([main, rest, jnp.zeros((BLK - 4, width), jnp.bfloat16)], axis=0)
    got_grad = exchange((validity * grad_resid).astype(jnp.bfloat16), back_order, extra)
    plan.done("norm4", sum_grad_attn.far)
    plan.done("deal", got_grad)
    got_grad = plan.before("unpack", got_grad)
    extra = got_grad[:, per_pair * BLK :].astype(jnp.float32)
    gains = sum_over(jnp.sum(extra[:, :2] + extra[:, 2:4], axis=0), "narrow", lane_count)
    output = unpack(got_output, send_place)
    grad_tokens = unpack(got_grad, send_place)
    (sum_wd,) = plan.rings["r"].finish()
    sum_wg, sum_wu = plan.rings["e"].finish()
    (sum_wo,) = plan.rings["f"].finish()
    (sum_wqkv,) = plan.rings["u"].finish()
    return (
        output,
        grad_tokens,
        gains[0],
        gains[1],
        sum_wqkv[:, :features],
        sum_wqkv[:, features : 2 * features],
        sum_wqkv[:, 2 * features :],
        sum_wo.T,
        sum_wg,
        sum_wu,
        sum_wd.T,
    )


def solution(mesh):
    placed = (
        P(("wide", "narrow"), None),
        P(),
        P(),
        P("wide", "narrow"),
        P("wide", "narrow"),
        P("wide", "narrow"),
        P("narrow", "wide"),
        P("wide", "narrow"),
        P("wide", "narrow"),
        P("narrow", "wide"),
        P(("wide", "narrow"), None),
        P(),
        P(),
    )
    return jax.shard_map(
        body,
        mesh=mesh,
        in_specs=placed,
        out_specs=(
            P(("wide", "narrow"), None),
            P(("wide", "narrow"), None),
            P(),
            P(),
            P("wide", "narrow"),
            P("wide", "narrow"),
            P("wide", "narrow"),
            P("narrow", "wide"),
            P("wide", "narrow"),
            P("wide", "narrow"),
            P("narrow", "wide"),
        ),
        check_vma=False,
    )
```

```python
import math

import jax
import jax.numpy as jnp
from jax import lax
from jax.experimental import pallas as pl
from jax.experimental.layout import Layout, with_layout_constraint
from jax.experimental.pallas import tpu as pltpu
from jax.sharding import PartitionSpec as P

HEAD_DIM = 64
MB = 2
BLK = 8
UNIT = 64


BRANCH = 1.4 / math.sqrt(40.0)
EPSILON = 1e-05
NEGATIVE = -1e30
RING_MAX = 8
RING_MAX = 8


def ring_rank(place, count):
    place = lax.rem(place + 2 * count, count)
    return jnp.where(place < count // 2, 2 * place, 2 * count - 1 - 2 * place)


def ring_place(rank, count):
    return jnp.where(rank % 2 == 0, rank // 2, count - 1 - rank // 2)


def ring_send(block, count, direction):
    order = list(range(0, count, 2)) + list(range(count - 1, 0, -2))
    route = [(order[i], order[(i + direction) % count]) for i in range(count)]
    return lax.ppermute(block, "wide", route)


def after(value, *others):
    return lax.optimization_barrier((value,) + others)[0] if others else value


class Order:
    def __init__(self):
        self.marks = ()

    def tie(self, value):
        return after(value, *self.marks)

    def at(self, *marks):
        self.marks = tuple(marks)

    def land(self, *arrived):
        self.marks = self.marks + tuple(arrived)


PLAN = {'r1': 'wd', 'r2': 'split', 'r3': 'da2', 'r4': 'wu', 'e1': 'wu', 'e2': 'far3', 'e3': 'both3', 'e4': 'back2', 'u1': 'wqkv', 'u2': 'da1', 'u3': 'norm4', 'o1': '@q3', 'g1': '@o3', 'd1': '@g3', 'C': 'attend1', 'O': 'da1', 'P6': 1, 'W': 'wqkv', 'f1': 'wo', 'f2': 'da1', 'f3': 'norm4', 'f4': 'deal'}
LAND = {'r1': 'da2', 'r2': 'wg', 'r3': 'yf', 'r4': 'both3', 'e1': 'both3', 'e2': 'mixed', 'e3': 'back1', 'e4': 'da1', 'u1': 'sum4', 'u3': 'unpack', 'f1': 'sum4', 'f2': 'norm4', 'f3': 'unpack'}
MADE = {'e4': 'back1', 'e2': 'gather3'}


class Plan:
    def __init__(self, order):
        self.order, self.rings, self.sent = order, {}, {}
        self.passed = set()

    def add(self, name, ring):
        self.rings[name], self.sent[name] = ring, 0
        self.push(())

    def push(self, marks):
        for name, ring in self.rings.items():
            while self.sent[name] < ring.count // 2:
                step = PLAN.get(name + str(self.sent[name] + 1))
                if step is not None and step[0] == "@":
                    if self.sent.get(step[1], 0) < int(step[2]):
                        break
                    self.order.at(*self.hop(step[1:]))
                elif step is not None and step not in self.passed:
                    break
                else:
                    self.order.at(*(marks if step is not None else ()))
                ring.send(self.order)
                self.sent[name] += 1
        self.order.at()

    def hop(self, name):
        hops = self.rings[name[0]].hops
        return hops[int(name[1]) - 1] if hops else ()

    def done(self, step, *marks):
        self.passed.add(step)
        self.push(marks)

    def before(self, step, value):
        marks = []
        for name, ready in LAND.items():
            if ready == step and self.sent.get(name[0], 0) >= int(name[1]):
                marks += self.hop(name)
        for name, ready in MADE.items():
            if ready == step and self.sent.get(name[0], 0) >= int(name[1]):
                messages = self.rings[name[0]].messages
                marks += messages[int(name[1]) - 1] if messages else ()
        return after(value, *marks)


class RingGather:
    def __init__(self, group, count):
        self.group, self.count, self.hops, self.messages = group, count, [], []
        self.block = jnp.concatenate(group, axis=0) if len(group) > 1 else group[0]

    def send(self, order):
        if self.count > RING_MAX:
            return
        up, down = self.hops[-1] if self.hops else (self.block, self.block)
        if len(self.hops) == self.count // 2 - 1:
            half = self.block.shape[0] // 16 * 8
            up, down = up[:half], down[half:]
            order.land(up, down)
        up, down = order.tie(up), order.tie(down)
        self.messages.append((up, down))
        self.hops.append((ring_send(up, self.count, 1), ring_send(down, self.count, -1)))

    def arrived(self):
        return self.hops[-1] if self.hops else ()

    def hop(self, index):
        return self.hops[index] if self.hops else ()

    def all(self, order):
        for _ in range(self.count // 2):
            self.send(order)
            order.at()

    def gathered(self):
        rows = self.group[0].shape[0]
        if not self.hops:
            fulls = [lax.all_gather(one, "wide", axis=0, tiled=True) for one in self.group]
            return [([full], [(0, 0, full.shape[0], None, 0)], rows) for full in fulls]
        far = self.count // 2
        found = []
        for step, (up, down) in enumerate(self.hops[:-1], 1):
            found += [(-step, 0, up), (step, 0, down)]
        up, down = self.hops[-1]
        found += [(far, 0, up), (far, up.shape[0], down)]
        out = []
        for index, own in enumerate(self.group):
            arrays, moves = [own], [(0, 0, rows, 0, 0)]
            first = index * rows
            for shift, start, piece in found:
                low = max(first, start)
                high = min(first + rows, start + piece.shape[0])
                if low < high:
                    arrays.append(piece)
                    moves.append((len(arrays) - 1, low - start, high - low, shift, low - first))
            out.append((arrays, moves, rows))
        return out


class RingSum:
    def __init__(self, fulls, count, where):
        self.fulls, self.count, self.where = fulls, count, where
        self.rows = fulls[0].shape[0] // count
        self.last = ()
        self.hops, self.messages = [], []
        self.hop = 0
        self.place = ring_place(lax.axis_index("wide"), count)
        self.half = self.rows * len(fulls) // 16 * 8

    def arrived(self):
        return self.last

    def local(self, shift):
        owner = ring_rank(self.place + shift, self.count)
        return jnp.concatenate(
            [
                lax.dynamic_slice_in_dim(full, owner * self.rows, self.rows, axis=0)
                for full in self.fulls
            ],
            axis=0,
        )

    def send(self, order):
        if self.count > RING_MAX:
            return
        self.hop += 1
        far, half = self.count // 2, self.half
        if self.hop == 1:
            both = self.local(far)
            up, down = order.tie(both[:half]), order.tie(both[half:])
        else:
            up, down = ring_add(
                self.where, self.count, far - self.hop + 1, self.fulls,
                order.tie(self.last[0]), self.last[1],
            )
        self.messages.append((up, down))
        self.last = (ring_send(up, self.count, 1), ring_send(down, self.count, -1))
        self.hops.append(self.last)

    def finish(self):
        if self.count > RING_MAX:
            return [
                lax.psum_scatter(full, "wide", scatter_dimension=0, tiled=True).astype(jnp.float32)
                for full in self.fulls
            ]
        up, down = self.last
        done = (
            self.local(0).astype(jnp.float32) + up.astype(jnp.float32) + down.astype(jnp.float32)
        )
        return [done[i * self.rows : (i + 1) * self.rows] for i in range(len(self.fulls))]


def swap_chip(block):
    return lax.ppermute(block, "narrow", [(0, 2), (1, 3), (2, 0), (3, 1)])


def swap_core(block):
    return lax.ppermute(block, "narrow", [(0, 1), (1, 0), (2, 3), (3, 2)])


class LaneGather:
    def __init__(self, block, order):
        self.block = order.tie(block)
        self.chip = swap_chip(self.block)
        self.core = swap_core(self.block)

    def finish(self, order):
        self.pieces = [self.block, self.core, self.chip, swap_core(order.tie(self.chip))]
        return self.pieces

    def whole(self):
        lane = lax.axis_index("narrow")
        full = jnp.zeros((4,) + self.block.shape, self.block.dtype)
        for index, piece in enumerate(self.pieces):
            full = lax.dynamic_update_slice(
                full, piece[None], (lane ^ index,) + (0,) * self.block.ndim
            )
        return full


class LaneSum:
    def __init__(self, own, across, pair, order):
        self.own, self.across = own, across
        self.got = swap_core(order.tie(pair))

    def cross(self, order):
        both = self.across.astype(jnp.float32) + self.got[0].astype(jnp.float32)
        both = order.tie(both.astype(jnp.bfloat16))
        order.land(both)
        self.far = swap_chip(both)

    def finish(self):
        return (
            self.own.astype(jnp.float32)
            + self.got[1].astype(jnp.float32)
            + self.far.astype(jnp.float32)
        )


def sum_over(value, axis, count):
    step = 1
    while step < count:
        value = value + lax.ppermute(value, axis, [(i, i ^ step) for i in range(count)])
        step *= 2
    return value


def angles(position):
    lane = jnp.arange(2 * HEAD_DIM, dtype=jnp.int32) % HEAD_DIM
    counter = (lane % (HEAD_DIM // 2)).astype(jnp.float32)
    frequency = jnp.exp(counter * (-2.0 * math.log(10000.0) / HEAD_DIM))
    phase_angle = position.astype(jnp.float32)[:, None] * frequency[None, :]
    sign = jnp.where(lane < HEAD_DIM // 2, -1.0, 1.0)
    return jnp.cos(phase_angle), jnp.sin(phase_angle) * sign[None, :]


def turn(field_in, cosine, sine, direction):
    rows, width = field_in.shape
    parts = []
    for low in range(0, width, 2 * HEAD_DIM):
        size = min(2 * HEAD_DIM, width - low)
        piece = field_in[:, low : low + size]
        if size < 2 * HEAD_DIM:
            piece = jnp.concatenate([piece, piece], axis=1)
        lane = lax.broadcasted_iota(jnp.int32, piece.shape, 1)
        swapped = jnp.where(
            lane % HEAD_DIM < HEAD_DIM // 2,
            pltpu.roll(piece, 2 * HEAD_DIM - HEAD_DIM // 2, 1),
            pltpu.roll(piece, HEAD_DIM // 2, 1),
        )
        parts.append((piece * cosine + direction * (swapped * sine))[:, :size])
    return jnp.concatenate(parts, axis=1)


def row_major(value):
    return with_layout_constraint(value, Layout(major_to_minor=tuple(range(value.ndim))))


def contract_rows(left, right):
    product = lax.dot_general(
        left, right, (((0,), (0,)), ((), ())), preferred_element_type=jnp.float32
    )
    return row_major(product.astype(jnp.bfloat16))


def times(left, right):
    return jnp.dot(left, right, preferred_element_type=jnp.float32)


def times_transpose(left, right):
    return lax.dot_general(
        left, right, (((1,), (1,)), ((), ())), preferred_element_type=jnp.float32
    )


def norm_rate(resid):
    return lax.rsqrt(jnp.mean(resid * resid, axis=1, keepdims=True) + EPSILON)


def norm_backward(grad_in, resid, rate, gain):
    scaled_grad = grad_in * gain[None, :]
    return rate * scaled_grad - resid * rate**3 * jnp.mean(
        scaled_grad * resid, axis=1, keepdims=True
    )


def invert_order(placing):
    counter = jnp.arange(placing.shape[0], dtype=jnp.int32)
    return jnp.sum(jnp.where(placing[None, :] == counter[:, None], counter[None, :], 0), axis=1)


def deal_routes(deal, my_rank, my_lane, rank_count, lane_count, block_count):
    per_pair = block_count // rank_count
    base_block = (my_rank * lane_count + my_lane) * block_count
    counter = jnp.arange(block_count, dtype=jnp.int32)
    every_block = jnp.arange(deal.shape[0], dtype=jnp.int32)
    owned = base_block + counter
    target = jnp.sum(jnp.where(deal[None, :] == owned[:, None], every_block[None, :], 0), axis=1)
    target_rank = target // (lane_count * block_count)
    target_slot = target % block_count
    earlier = (target_rank[None, :] == target_rank[:, None]) & (
        target_slot[None, :] < target_slot[:, None]
    )
    send_place = target_rank * per_pair + jnp.sum(earlier.astype(jnp.int32), axis=1)
    mine = lax.dynamic_slice_in_dim(deal, base_block, block_count)
    source_rank = mine // (lane_count * block_count)
    before = (source_rank[None, :] == source_rank[:, None]) & (counter[None, :] < counter[:, None])
    recv_place = source_rank * per_pair + jnp.sum(before.astype(jnp.int32), axis=1)
    return (send_place, recv_place)


def stream_layout(length_row, my_rank, slot_rows):
    extent = (length_row + UNIT - 1) // UNIT * UNIT
    begin = jnp.cumsum(extent) - extent
    places = my_rank * slot_rows - slot_rows + jnp.arange(2 * slot_rows, dtype=jnp.int32)
    ending = begin + length_row
    inside = (places[:, None] >= begin[None, :]) & (places[:, None] < ending[None, :])
    number = jnp.arange(length_row.shape[0], dtype=jnp.int32) + 1
    segment = jnp.sum(jnp.where(inside, number[None, :], 0), axis=1) - 1
    position = places - jnp.sum(jnp.where(inside, begin[None, :], 0), axis=1)
    return (segment, position)


VMEM_LIMIT = 60 * 1024 * 1024


def dot_nn(left, right):
    return jnp.dot(left, right, preferred_element_type=jnp.float32)


def dot_nt(left, right):
    return times_transpose(left, right)


def dot_tn(left, right):
    return lax.dot_general(
        left, right, (((0,), (0,)), ((), ())), preferred_element_type=jnp.float32
    )


def params():
    return pltpu.CompilerParams(vmem_limit_bytes=VMEM_LIMIT)


def cost(flops, bytes_accessed, transcendentals=0):
    return pl.CostEstimate(
        flops=flops, bytes_accessed=bytes_accessed, transcendentals=transcendentals
    )


ANY = pl.BlockSpec(memory_space=pl.ANY)


class Collector:
    def __init__(self, gathered):
        self.arrays, self.moves, self.rows = gathered
        self.height = self.rows * lax.axis_size("wide")
        self.width = self.arrays[0].shape[1]
        self.shape = jax.ShapeDtypeStruct((self.height, self.width), jnp.bfloat16)

    def scratch(self):
        return [
            pltpu.VMEM((self.height, self.width), jnp.bfloat16),
            pltpu.SemaphoreType.DMA((len(self.moves) + 1,)),
        ]

    def copies(self, where, refs, whole, sems):
        count = self.height // self.rows
        for index, (array, start, rows, shift, offset) in enumerate(self.moves):
            row = offset
            if shift is not None:
                owner = ring_rank(ring_place(where[2], count) + shift, count)
                row = pl.multiple_of(owner * self.rows + offset, 16)
            yield pltpu.make_async_copy(
                refs[array].at[pl.ds(start, rows), :], whole.at[pl.ds(row, rows), :], sems.at[index]
            )

    def start(self, *args):
        for copy in self.copies(*args):
            copy.start()

    def wait(self, *args):
        for copy in self.copies(*args):
            copy.wait()

    def out(self, whole, out_ref, sems):
        return pltpu.make_async_copy(whole, out_ref, sems.at[len(self.moves)])


class Lanes:
    def __init__(self, pieces):
        self.pieces = list(pieces)
        self.block = pieces[0].shape
        self.shape = jax.ShapeDtypeStruct((4,) + self.block, jnp.bfloat16)

    def scratch(self):
        return [pltpu.VMEM((4,) + self.block, jnp.bfloat16), pltpu.SemaphoreType.DMA((4,))]

    def start(self, refs, rows, sems):
        for index in range(4):
            pltpu.make_async_copy(refs[index], rows.at[index], sems.at[index]).start()

    def wait(self, step, refs, rows, sems):
        pltpu.make_async_copy(refs[0], rows.at[step], sems.at[step]).wait()


def by_lane(rows, width):
    return pl.BlockSpec((None, rows, width), lambda i, where: (where[0] ^ i, 0, 0))


def fixed(*shape):
    return pl.BlockSpec(shape, lambda i, where: (0,) * len(shape))


def whole(*shape):
    return pl.BlockSpec(
        shape, lambda i, where: (0,) * len(shape), pipeline_mode=pl.Buffered(1)
    )


def by_parity(parity, both):
    half = both.shape[0] // 2
    low, high = both[:half], both[half:]
    return jnp.where(parity == 0, low, high), jnp.where(parity == 0, high, low)


def project_kernel(weight, lanes, where, *refs):
    count = len(weight.arrays)
    weights, refs = refs[:count], refs[count:]
    pieces, refs = refs[:4], refs[4:]
    cos_ref, sin_ref, q_ref, send_ref, keep_ref, w_out, rows_out, w, w_sems, rows, r_sems, o_sems = refs
    skip = weight.width - 3 * q_ref.shape[-1]
    step = pl.program_id(0)

    @pl.when(step == 0)
    def _():
        lanes.start(pieces, rows, r_sems)
        weight.start(where, weights, w, w_sems)
        weight.wait(where, weights, w, w_sems)
        weight.out(w, w_out, w_sems).start()

    lanes.wait(step, pieces, rows, r_sems)
    pltpu.make_async_copy(rows.at[step], rows_out.at[where[0] ^ step], o_sems.at[step]).start()
    width = q_ref.shape[-1]
    z = dot_nn(rows[step], w[:, skip:])
    turned = turn(z[:, : 2 * width], cos_ref[...], sin_ref[...], 1.0)
    first, second = by_parity(where[1], turned[:, :width])
    q_ref[0], q_ref[1] = first.astype(jnp.bfloat16), second.astype(jnp.bfloat16)
    first, second = by_parity(where[1], pack_pair(turned[:, width:], z[:, 2 * width :]))
    send_ref[...], keep_ref[...] = first.astype(jnp.bfloat16), second.astype(jnp.bfloat16)

    @pl.when(step == 3)
    def _():
        weight.out(w, w_out, w_sems).wait()
        for index in range(4):
            pltpu.make_async_copy(rows.at[index], rows_out.at[index], o_sems.at[index]).wait()


def project(where, gathered, width, pieces, cosine, sine):
    weight, lanes = Collector(gathered), Lanes(pieces)
    count, depth = lanes.block
    angle = by_lane(count, 2 * HEAD_DIM)
    pair = pl.BlockSpec((2, None, count // 2, width), lambda i, where: (0, where[0] ^ i, 0, 0))
    out = jax.ShapeDtypeStruct((2, 4, count // 2, width), jnp.bfloat16)
    both = jax.ShapeDtypeStruct((4, count // 2, 2 * width), jnp.bfloat16)
    both_spec = by_lane(count // 2, 2 * width)
    return pl.pallas_call(
        lambda *refs: project_kernel(weight, lanes, *refs),
        out_shape=(out, both, both, weight.shape, lanes.shape),
        grid_spec=pltpu.PrefetchScalarGridSpec(
            num_scalar_prefetch=1,
            grid=(4,),
            in_specs=[ANY] * (len(weight.arrays) + 4) + [angle, angle],
            out_specs=(pair, both_spec, both_spec, ANY, ANY),
            scratch_shapes=weight.scratch() + lanes.scratch() + [pltpu.SemaphoreType.DMA((4,))],
        ),
        compiler_params=params(),
        cost_estimate=cost(8 * count * depth * 3 * width, 40 * count * depth),
        name="project",
    )(where, *weight.arrays, *lanes.pieces, cosine, sine)


def put_relative(step, value, own_ref, across_ref, pair_ref):
    @pl.when(step == 0)
    def _():
        own_ref[...] = value

    @pl.when(step == 2)
    def _():
        across_ref[...] = value

    @pl.when(step == 3)
    def _():
        pair_ref[0] = value

    @pl.when(step == 1)
    def _():
        pair_ref[1] = value


def relative_out(rows, width):
    shapes = (
        jax.ShapeDtypeStruct((rows, width), jnp.bfloat16),
        jax.ShapeDtypeStruct((rows, width), jnp.bfloat16),
        jax.ShapeDtypeStruct((2, rows, width), jnp.bfloat16),
    )
    specs = (whole(rows, width), whole(rows, width), whole(2, rows, width))
    return shapes, specs


def part_of(weight, width):
    columns = width if weight.shape[1] == width else (width + 127) // 128 * 128
    return pl.BlockSpec(
        (weight.shape[0], columns), lambda i, where: (0, 0), pipeline_mode=pl.Buffered(1)
    )


def merge_kernel(weight, where, *refs):
    count = len(weight.arrays)
    weights, refs = refs[:count], refs[count:]
    a_ref, b_ref, own_ref, across_ref, pair_ref, o_ref, w_out, w, w_sems = refs
    step = pl.program_id(0)

    @pl.when(step == 0)
    def _():
        weight.start(where, weights, w, w_sems)
        weight.wait(where, weights, w, w_sems)
        weight.out(w, w_out, w_sems).start()

    low, high = by_parity(where[1], jnp.concatenate([a_ref[...], b_ref[...]], axis=0))
    rows = jnp.concatenate([low, high], axis=0)
    o_ref[...] = rows
    put_relative(step, dot_nt(rows, w[...]).astype(jnp.bfloat16), own_ref, across_ref, pair_ref)

    @pl.when(step == 3)
    def _():
        weight.out(w, w_out, w_sems).wait()


def merge(where, gathered, first, second):
    weight = Collector(gathered)
    lanes, rows, width = first.shape
    shapes, specs = relative_out(2 * rows, weight.height)
    return pl.pallas_call(
        lambda *refs: merge_kernel(weight, *refs),
        out_shape=shapes + (jax.ShapeDtypeStruct((lanes, 2 * rows, width), jnp.bfloat16), weight.shape),
        grid_spec=pltpu.PrefetchScalarGridSpec(
            num_scalar_prefetch=1,
            grid=(4,),
            in_specs=[ANY] * len(weight.arrays) + [by_lane(rows, width)] * 2,
            out_specs=specs + (by_lane(2 * rows, width), ANY),
            scratch_shapes=weight.scratch(),
        ),
        compiler_params=params(),
        cost_estimate=cost(16 * rows * width * weight.height, 20 * rows * weight.height),
        name="merge",
    )(where, *weight.arrays, first, second)


def hidden_kernel(gate_w, up_w, lanes, where, *refs):
    gates, refs = refs[: len(gate_w.arrays)], refs[len(gate_w.arrays) :]
    ups, refs = refs[: len(up_w.arrays)], refs[len(up_w.arrays) :]
    pieces, refs = refs[:4], refs[4:]
    gate_ref, up_ref, hidden_ref, g_out, u_out, rows_out, g, g_sems, u, u_sems, rows, r_sems, o_sems = refs
    step = pl.program_id(0)

    @pl.when(step == 0)
    def _():
        lanes.start(pieces, rows, r_sems)
        gate_w.start(where, gates, g, g_sems)
        up_w.start(where, ups, u, u_sems)
        gate_w.wait(where, gates, g, g_sems)
        gate_w.out(g, g_out, g_sems).start()

    lanes.wait(step, pieces, rows, r_sems)
    pltpu.make_async_copy(rows.at[step], rows_out.at[where[0] ^ step], o_sems.at[step]).start()
    gate = dot_nn(rows[step], g[...])
    gate_ref[...] = gate

    @pl.when(step == 0)
    def _():
        up_w.wait(where, ups, u, u_sems)
        up_w.out(u, u_out, u_sems).start()

    up = dot_nn(rows[step], u[...])
    up_ref[...] = up
    hidden_ref[...] = (gate * jax.nn.sigmoid(gate) * up).astype(jnp.bfloat16)

    @pl.when(step == 3)
    def _():
        gate_w.out(g, g_out, g_sems).wait()
        up_w.out(u, u_out, u_sems).wait()
        for index in range(4):
            pltpu.make_async_copy(rows.at[index], rows_out.at[index], o_sems.at[index]).wait()


def hidden_units(where, gathered_gate, gathered_up, pieces):
    gate_w, up_w, lanes = Collector(gathered_gate), Collector(gathered_up), Lanes(pieces)
    rows, depth = lanes.block
    width = gate_w.width
    wide = jax.ShapeDtypeStruct((4, rows, width), jnp.float32)
    return pl.pallas_call(
        lambda *refs: hidden_kernel(gate_w, up_w, lanes, *refs),
        out_shape=(
            wide, wide, jax.ShapeDtypeStruct((4, rows, width), jnp.bfloat16),
            gate_w.shape, up_w.shape, lanes.shape,
        ),
        grid_spec=pltpu.PrefetchScalarGridSpec(
            num_scalar_prefetch=1,
            grid=(4,),
            in_specs=[ANY] * (len(gate_w.arrays) + len(up_w.arrays) + 4),
            out_specs=(by_lane(rows, width),) * 3 + (ANY,) * 3,
            scratch_shapes=gate_w.scratch() + up_w.scratch() + lanes.scratch()
            + [pltpu.SemaphoreType.DMA((4,))],
        ),
        compiler_params=params(),
        cost_estimate=cost(16 * rows * depth * width, 60 * rows * width, 4 * rows * width),
        name="hidden_units",
    )(where, *gate_w.arrays, *up_w.arrays, *lanes.pieces)


def split_kernel(down_w, where, *refs):
    downs, refs = refs[: len(down_w.arrays)], refs[len(down_w.arrays) :]
    cot_ref, gate_ref, up_ref, dg_ref, du_ref, d_out, d, d_sems = refs
    step = pl.program_id(0)

    @pl.when(step == 0)
    def _():
        down_w.start(where, downs, d, d_sems)
        down_w.wait(where, downs, d, d_sems)
        down_w.out(d, d_out, d_sems).start()

    grad = dot_nn(cot_ref[...], d[...])
    gate, up = gate_ref[...], up_ref[...]
    sigma = jax.nn.sigmoid(gate)
    part = grad * sigma
    dg_ref[...] = (part * up * (1.0 + gate * (1.0 - sigma))).astype(jnp.bfloat16)
    du_ref[...] = (part * gate).astype(jnp.bfloat16)

    @pl.when(step == 3)
    def _():
        down_w.out(d, d_out, d_sems).wait()


def split_grads(where, gathered, cot, gate, up):
    down_w = Collector(gathered)
    lanes, rows, width = gate.shape
    depth = cot.shape[2]
    narrow = jax.ShapeDtypeStruct(gate.shape, jnp.bfloat16)
    block = by_lane(rows, width)
    return pl.pallas_call(
        lambda *refs: split_kernel(down_w, *refs),
        out_shape=(narrow, narrow, down_w.shape),
        grid_spec=pltpu.PrefetchScalarGridSpec(
            num_scalar_prefetch=1,
            grid=(4,),
            in_specs=[ANY] * len(down_w.arrays) + [by_lane(rows, depth), block, block],
            out_specs=(block, block, ANY),
            scratch_shapes=down_w.scratch(),
        ),
        compiler_params=params(),
        cost_estimate=cost(8 * rows * depth * width, 60 * rows * width, 4 * rows * width),
        name="split_grads",
    )(where, *down_w.arrays, cot, gate, up)


def terms_kernel(count, where, *refs):
    total = None
    for index in range(count):
        rows, weight = refs[index][...], refs[count + index]
        term = dot_nt(rows, weight[:, weight.shape[1] - rows.shape[1] :])
        total = term if total is None else total + term
    put_relative(pl.program_id(0), total.astype(jnp.bfloat16), *refs[2 * count :])


def terms(where, pairs):
    rows = pairs[0][0].shape[1]
    height = pairs[0][1].shape[0]
    shapes, specs = relative_out(rows, height)
    depth = sum(weight.shape[1] for _, weight in pairs)
    return pl.pallas_call(
        lambda *refs: terms_kernel(len(pairs), *refs),
        out_shape=shapes,
        grid_spec=pltpu.PrefetchScalarGridSpec(
            num_scalar_prefetch=1,
            grid=(4,),
            in_specs=[by_lane(rows, one.shape[2]) for one, _ in pairs]
            + [whole(*weight.shape) for _, weight in pairs],
            out_specs=specs,
        ),
        compiler_params=params(),
        cost_estimate=cost(8 * rows * height * depth, 2 * (4 * rows + height) * depth),
        name="terms",
    )(where, *[one for one, _ in pairs], *[weight for _, weight in pairs])


def mixed_kernel(lanes, where, *refs):
    pieces, refs = refs[:4], refs[4:]
    w_ref, out_ref, rows_out, rows, r_sems, o_sems = refs
    step = pl.program_id(0)

    @pl.when(step == 0)
    def _():
        lanes.start(pieces, rows, r_sems)

    lanes.wait(step, pieces, rows, r_sems)
    pltpu.make_async_copy(rows.at[step], rows_out.at[where[0] ^ step], o_sems.at[step]).start()
    out = dot_nn(rows[step], w_ref[:, : out_ref.shape[-1]])
    first, second = by_parity(where[1], out)
    out_ref[0], out_ref[1] = first.astype(jnp.bfloat16), second.astype(jnp.bfloat16)

    @pl.when(step == 3)
    def _():
        for index in range(4):
            pltpu.make_async_copy(rows.at[index], rows_out.at[index], o_sems.at[index]).wait()


def mixed_grads(where, weight, width, pieces):
    lanes = Lanes(pieces)
    count, depth = lanes.block
    return pl.pallas_call(
        lambda *refs: mixed_kernel(lanes, *refs),
        out_shape=(jax.ShapeDtypeStruct((2, 4, count // 2, width), jnp.bfloat16), lanes.shape),
        grid_spec=pltpu.PrefetchScalarGridSpec(
            num_scalar_prefetch=1,
            grid=(4,),
            in_specs=[ANY] * 4 + [part_of(weight, width)],
            out_specs=(
                pl.BlockSpec((2, None, count // 2, width), lambda i, where: (0, where[0] ^ i, 0, 0)),
                ANY,
            ),
            scratch_shapes=lanes.scratch() + [pltpu.SemaphoreType.DMA((4,))],
        ),
        compiler_params=params(),
        cost_estimate=cost(8 * count * depth * width, 20 * count * depth),
        name="mixed_grads",
    )(where, *lanes.pieces, weight)


def ring_add_kernel(count, split, where, *refs):
    ups, downs, refs = refs[:count], refs[count : 2 * count], refs[2 * count :]
    up_in, down_in, up_out, down_out = refs
    step = pl.program_id(0)
    for index in range(count):

        @pl.when(step // 2 == index)
        def _():
            up = ups[index][...].astype(jnp.float32)
            down = downs[index][...].astype(jnp.float32)
            if split:
                up = jnp.where(step < count, up + up_in[...].astype(jnp.float32), up)
                down = jnp.where(step < count, down, down + down_in[...].astype(jnp.float32))
            else:
                up = up + up_in[...].astype(jnp.float32)
                down = down + down_in[...].astype(jnp.float32)
            up_out[...] = up.astype(jnp.bfloat16)
            down_out[...] = down.astype(jnp.bfloat16)


def ring_add(where, ranks, shift, fulls, up, down):
    count = len(fulls)
    rows, width = fulls[0].shape[0] // ranks, fulls[0].shape[1]
    part = rows // 2
    split = up.shape[0] < rows * count

    def local(index, direction):
        def at(i, where):
            owner = ring_rank(ring_place(where[2], ranks) + direction * shift, ranks)
            return (owner * 2 + jnp.clip(i - 2 * index, 0, 1), 0)

        return pl.BlockSpec((part, width), at)

    block = pl.BlockSpec((part, width), lambda i, where: (i, 0))
    upper, lower = block, block
    if split:
        upper = pl.BlockSpec((part, width), lambda i, where: (jnp.minimum(i, count - 1), 0))
        lower = pl.BlockSpec((part, width), lambda i, where: (jnp.maximum(i - count, 0), 0))
    out = jax.ShapeDtypeStruct((rows * count, width), jnp.bfloat16)
    return pl.pallas_call(
        lambda *refs: ring_add_kernel(count, split, *refs),
        out_shape=(out, out),
        grid_spec=pltpu.PrefetchScalarGridSpec(
            num_scalar_prefetch=1,
            grid=(2 * count,),
            in_specs=[local(index, 1) for index in range(count)]
            + [local(index, -1) for index in range(count)]
            + [upper, lower],
            out_specs=(block, block),
        ),
        compiler_params=params(),
        cost_estimate=cost(4 * rows * count * width, 12 * rows * count * width),
        name="ring_add",
    )(where, *fulls, *fulls, up, down)


def fill_bias(seg_col_ref, seg_row_ref, bias_own, bias_prev):
    slot = bias_own.shape[0]
    query = seg_row_ref[...]
    key = lax.broadcasted_iota(jnp.int32, (slot, slot), 0)
    place = lax.broadcasted_iota(jnp.int32, (slot, slot), 1)
    own = seg_col_ref[slot:, :]
    allowed = (own == query) & (query >= 0) & (key <= place) | (key == place)
    bias_own[...] = jnp.where(allowed, 0.0, NEGATIVE)
    if bias_prev is not None:
        before = seg_col_ref[:slot, :]
        bias_prev[...] = jnp.where((before == query) & (query >= 0), 0.0, NEGATIVE)


def over_pairs(width, body):
    pairs = width // (2 * HEAD_DIM)

    def step(index, carry):
        body(pl.multiple_of(index * 2 * HEAD_DIM, 2 * HEAD_DIM), index * 2, 2)
        return carry

    lax.fori_loop(0, pairs, step, 0)
    if width % (2 * HEAD_DIM):
        body(pairs * 2 * HEAD_DIM, pairs * 2, 1)


def head_mask(lanes, head, value):
    lane = lax.broadcasted_iota(jnp.int32, (1, lanes), 1)
    return jnp.where(lane // HEAD_DIM == head, value, 0.0).astype(jnp.bfloat16)


def flat(ref, low, lanes):
    value = ref[:, :, pl.ds(low, lanes)]
    return value.reshape(value.shape[0] * value.shape[1], lanes)


def pack_pair(keys, values):
    even = keys.shape[1] // (2 * HEAD_DIM) * 2 * HEAD_DIM
    return jnp.concatenate(
        [keys[:, :even], values[:, :even], keys[:, even:], values[:, even:]], axis=1
    )


def split_pair(both):
    width = both.shape[1] // 2
    even = width // (2 * HEAD_DIM) * 2 * HEAD_DIM
    odd = width - even
    return (
        jnp.concatenate([both[:, :even], both[:, 2 * even : 2 * even + odd]], axis=1),
        jnp.concatenate([both[:, even : 2 * even], both[:, 2 * even + odd :]], axis=1),
    )


def pair_lane(low, heads, which, width):
    even = width // (2 * HEAD_DIM) * 2 * HEAD_DIM
    if heads == 2:
        return pl.multiple_of(low + which * even, 2 * HEAD_DIM)
    return 2 * even + which * HEAD_DIM


def attend_kernel(with_prev, seg_col_ref, seg_row_ref, q_ref, kv_ref, *refs):
    if with_prev:
        before_ref, o_ref, lse_ref, bias_own, bias_prev = refs
    else:
        o_ref, lse_ref, bias_own = refs
        bias_prev = None
    fill_bias(seg_col_ref, seg_row_ref, bias_own, bias_prev)
    slot = bias_own.shape[0]
    part = slot // 2

    def pair(low, head, heads):
        lanes = heads * HEAD_DIM
        q = flat(q_ref, low, lanes)
        at_k, at_v = (pair_lane(low, heads, which, q_ref.shape[2]) for which in range(2))
        k, v = flat(kv_ref, at_k, lanes), flat(kv_ref, at_v, lanes)
        if with_prev:
            kp, vp = flat(before_ref, at_k, lanes), flat(before_ref, at_v, lanes)
        for half in range(2):
            first, keys = half * part, (half + 1) * part
            mixed = []
            for one in range(heads):
                qm = q[first : first + part] * head_mask(lanes, one, 1.0 / math.sqrt(HEAD_DIM))
                s = dot_nt(k[:keys], qm) + bias_own[:keys, first : first + part]
                top = jnp.max(s, axis=0, keepdims=True)
                if with_prev:
                    sp = dot_nt(kp, qm) + bias_prev[:, first : first + part]
                    top = jnp.maximum(top, jnp.max(sp, axis=0, keepdims=True))
                p = jnp.exp(s - top)
                total = jnp.sum(p, axis=0, keepdims=True)
                o = dot_tn(v[:keys], p.astype(jnp.bfloat16))
                if with_prev:
                    pp = jnp.exp(sp - top)
                    total = total + jnp.sum(pp, axis=0, keepdims=True)
                    o = o + dot_tn(vp, pp.astype(jnp.bfloat16))
                mixed.append(o[one * HEAD_DIM : (one + 1) * HEAD_DIM] / total)
                lse_ref[pl.ds(head + one, 1), first : first + part] = top + jnp.log(total)
            o = jnp.concatenate(mixed, axis=0).T
            quarter = o_ref.shape[1]
            o_ref[first // quarter : (first + part) // quarter, :, pl.ds(low, lanes)] = (
                o.astype(jnp.bfloat16).reshape(part // quarter, quarter, lanes)
            )

    over_pairs(q_ref.shape[2], pair)


def attend(slot, seg_col, seg_row, q, kv, before=None):
    _, lanes, rows, width = q.shape
    count = lanes * rows
    heads = width // HEAD_DIM
    with_prev = before is not None
    both = pl.BlockSpec((lanes, rows, 2 * width), lambda i: (0, 0, 0))
    return pl.pallas_call(
        lambda *refs: attend_kernel(with_prev, *refs),
        out_shape=(
            jax.ShapeDtypeStruct((lanes, rows, width), jnp.bfloat16),
            jax.ShapeDtypeStruct((16, count), jnp.float32),
        ),
        grid=(1,),
        in_specs=slot_specs(slot, lanes, rows, width) + [both] * (2 if with_prev else 1),
        out_specs=(
            pl.BlockSpec((lanes, rows, width), lambda i: (0, 0, 0)),
            pl.BlockSpec((16, count), lambda i: (0, 0)),
        ),
        scratch_shapes=[pltpu.VMEM((count, count), jnp.float32)] * (2 if with_prev else 1),
        compiler_params=params(),
        cost_estimate=cost(
            (5 if with_prev else 2) * heads * count * count * 256,
            12 * count * width,
            heads * count * count,
        ),
        name="attend",
    )(seg_col, seg_row, q, kv, *([before] if with_prev else []))


def slot_specs(slot, lanes, rows, width):
    count = lanes * rows
    return [
        pl.BlockSpec((None, 2 * count, 1), lambda i: (slot, 0, 0)),
        pl.BlockSpec((None, 1, count), lambda i: (slot, 0, 0)),
        pl.BlockSpec((None, lanes, rows, width), lambda i: (slot, 0, 0, 0)),
    ]


def attend_back_kernel(
    with_prev, seg_col_ref, seg_row_ref, q_ref, kv_ref, o_ref, do_ref, lse_ref, *refs
):
    if with_prev:
        before_ref, dq_ref, dk_ref, dv_ref, back_ref, bias_own, bias_prev = refs
    else:
        dq_ref, dk_ref, dv_ref, bias_own = refs
        bias_prev = None
    fill_bias(seg_col_ref, seg_row_ref, bias_own, bias_prev)
    slot = bias_own.shape[0]
    part = slot // 2
    quarter = q_ref.shape[1]
    scale = 1.0 / math.sqrt(HEAD_DIM)

    def pair(low, head, heads):
        lanes = heads * HEAD_DIM
        q, o, do = (flat(ref, low, lanes) for ref in (q_ref, o_ref, do_ref))
        at_k, at_v = (pair_lane(low, heads, which, q_ref.shape[2]) for which in range(2))
        k, v = flat(kv_ref, at_k, lanes), flat(kv_ref, at_v, lanes)
        if with_prev:
            kp, vp = flat(before_ref, at_k, lanes), flat(before_ref, at_v, lanes)
        product = (do.astype(jnp.float32) * o.astype(jnp.float32)).T
        dk = [0.0, 0.0]
        dv = [0.0, 0.0]
        dkp = dvp = 0.0
        for half in range(2):
            first, keys = half * part, (half + 1) * part
            turned = []
            for one in range(heads):
                span = slice(one * HEAD_DIM, (one + 1) * HEAD_DIM)
                delta = jnp.sum(product[span, first : first + part], axis=0, keepdims=True)
                lse = lse_ref[pl.ds(head + one, 1), first : first + part]
                qm = q[first : first + part] * head_mask(lanes, one, scale)
                dm = do[first : first + part] * head_mask(lanes, one, 1.0)
                p = jnp.exp(dot_nt(k[:keys], qm) + bias_own[:keys, first : first + part] - lse)
                ds = (p * (dot_nt(v[:keys], dm) - delta)).astype(jnp.bfloat16)
                new_dv = dot_nn(p.astype(jnp.bfloat16), dm)
                new_dk = dot_nn(ds, qm)
                for index in range(half + 1):
                    rows = slice(index * part, (index + 1) * part)
                    dv[index] = dv[index] + new_dv[rows]
                    dk[index] = dk[index] + new_dk[rows]
                dq = dot_tn(k[:keys], ds)
                if with_prev:
                    p = jnp.exp(dot_nt(kp, qm) + bias_prev[:, first : first + part] - lse)
                    ds = (p * (dot_nt(vp, dm) - delta)).astype(jnp.bfloat16)
                    dvp = dvp + dot_nn(p.astype(jnp.bfloat16), dm)
                    dkp = dkp + dot_nn(ds, qm)
                    dq = dq + dot_tn(kp, ds)
                turned.append(dq[span])
            dq = jnp.concatenate(turned, axis=0).T * scale
            dq_ref[first // quarter : (first + part) // quarter, :, pl.ds(low, lanes)] = dq.reshape(
                part // quarter, quarter, lanes
            )
        for index in range(2):
            span = slice(index * part // quarter, (index + 1) * part // quarter)
            shape = (part // quarter, quarter, lanes)
            dk_ref[span, :, pl.ds(low, lanes)] = dk[index].reshape(shape)
            dv_ref[span, :, pl.ds(low, lanes)] = dv[index].reshape(shape)
        if with_prev:
            shape = (slot // quarter, quarter, lanes)
            back_ref[:, :, pl.ds(at_k, lanes)] = dkp.astype(jnp.bfloat16).reshape(shape)
            back_ref[:, :, pl.ds(at_v, lanes)] = dvp.astype(jnp.bfloat16).reshape(shape)

    over_pairs(q_ref.shape[2], pair)


def attend_back(slot, seg_col, seg_row, q, kv, o, do, lse_in, before=None):
    _, lanes, rows, width = q.shape
    count = lanes * rows
    heads = width // HEAD_DIM
    with_prev = before is not None
    both = pl.BlockSpec((lanes, rows, 2 * width), lambda i: (0, 0, 0))
    one = pl.BlockSpec((lanes, rows, width), lambda i: (0, 0, 0))
    specs = slot_specs(slot, lanes, rows, width)
    wide = jax.ShapeDtypeStruct((lanes, rows, width), jnp.float32)
    sent = jax.ShapeDtypeStruct((lanes, rows, 2 * width), jnp.bfloat16)
    return pl.pallas_call(
        lambda *refs: attend_back_kernel(with_prev, *refs),
        out_shape=(wide, wide, wide) + ((sent,) if with_prev else ()),
        grid=(1,),
        in_specs=specs
        + [both, one, specs[2], pl.BlockSpec((16, count), lambda i: (0, 0))]
        + ([both] if with_prev else []),
        out_specs=(one, one, one) + ((both,) if with_prev else ()),
        scratch_shapes=[pltpu.VMEM((count, count), jnp.float32)] * (2 if with_prev else 1),
        compiler_params=params(),
        cost_estimate=cost(
            (12 if with_prev else 5) * heads * count * count * 256,
            30 * count * width,
            heads * count * count,
        ),
        name="attend_back",
    )(seg_col, seg_row, q, kv, o, do, lse_in, *([before] if with_prev else []))


def join_kernel(where, *refs):
    dq_a, dk_a, dv_a, dq_b, dk_b, dv_b, back_ref, cos_ref, sin_ref, out_ref = refs
    cos_a, cos_b = by_parity(where[1], cos_ref[...])
    sin_a, sin_b = by_parity(where[1], sin_ref[...])
    dk_back, dv_back = split_pair(back_ref[...])
    dk = dk_a[...] + dk_back.astype(jnp.float32)
    dv = dv_a[...] + dv_back.astype(jnp.float32)
    first = jnp.concatenate(
        [turn(dq_a[...], cos_a, sin_a, -1.0), turn(dk, cos_a, sin_a, -1.0), dv], axis=1
    )
    second = jnp.concatenate(
        [turn(dq_b[...], cos_b, sin_b, -1.0), turn(dk_b[...], cos_b, sin_b, -1.0), dv_b[...]], axis=1
    )
    half = first.shape[0]
    out_ref[:half] = jnp.where(where[1] == 0, first, second).astype(jnp.bfloat16)
    out_ref[half:] = jnp.where(where[1] == 0, second, first).astype(jnp.bfloat16)


def join_grads(where, first, second, back, cosine, sine):
    lanes, rows, width = first[0].shape
    block = by_lane(rows, width)
    both = by_lane(rows, 2 * width)
    angle = by_lane(2 * rows, 2 * HEAD_DIM)
    return pl.pallas_call(
        join_kernel,
        out_shape=jax.ShapeDtypeStruct((lanes, 2 * rows, 3 * width), jnp.bfloat16),
        grid_spec=pltpu.PrefetchScalarGridSpec(
            num_scalar_prefetch=1,
            grid=(lanes,),
            in_specs=[block] * 6 + [both, angle, angle],
            out_specs=by_lane(2 * rows, 3 * width),
        ),
        compiler_params=params(),
        cost_estimate=cost(16 * lanes * rows * width, 44 * lanes * rows * width),
        name="join_grads",
    )(where, *first, *second, back, cosine, sine)


def to_next(block, count, direction):
    route = [(low, low + 1) for low in range(count - 1)]
    return lax.ppermute(block, "wide", [(b, a) for a, b in route] if direction < 0 else route)


def body(
    tokens,
    norm_attn,
    norm_ffn,
    w_query,
    w_key,
    w_value,
    w_out,
    w_gate,
    w_up,
    w_down,
    cotangent,
    lengths,
    deal,
):
    rank_count = lax.axis_size("wide")
    lane_count = lax.axis_size("narrow")
    my_rank = lax.axis_index("wide")
    my_lane = lax.axis_index("narrow")
    row_count = tokens.shape[0]
    width = tokens.shape[1]
    block_count = row_count // BLK
    per_pair = block_count // rank_count
    micro_rows = row_count // MB
    slot_rows = lane_count * micro_rows
    all_rows = lane_count * row_count
    features = w_query.shape[1]
    shard = w_query.shape[0]
    send_place, recv_place = deal_routes(
        deal, my_rank, my_lane, rank_count, lane_count, block_count
    )
    send_order = invert_order(send_place)
    back_order = invert_order(recv_place)

    def exchange(flat_rows, order_of, extra=None):
        packed = flat_rows.reshape(block_count, BLK, width)[order_of].reshape(
            rank_count, per_pair * BLK, width
        )
        if extra is not None:
            extra = jnp.broadcast_to(extra[None], (rank_count,) + extra.shape)
            packed = jnp.concatenate([packed, extra], axis=1)
        return lax.all_to_all(order.tie(packed), "wide", split_axis=0, concat_axis=0, tiled=True)

    def unpack(got, placing):
        rows = got[:, : per_pair * BLK]
        return rows.reshape(block_count, BLK, width)[placing].reshape(row_count, width)

    def rows_of(array):
        return array.reshape(all_rows, array.shape[-1])

    order = Order()
    plan = Plan(order)
    ring_qkv = RingGather([jnp.concatenate([w_query, w_key, w_value], axis=1)], rank_count)
    ring_out = RingGather([w_out.T], rank_count)
    ring_ffn = RingGather([w_gate, w_up], rank_count)
    ring_down = RingGather([w_down.T], rank_count)
    for name, ring in (("q", ring_qkv), ("o", ring_out), ("g", ring_ffn), ("d", ring_down)):
        plan.add(name, ring)

    got_x = exchange(tokens, send_order)
    plan.done("start")
    if "C" not in PLAN:
        got_cot = exchange(cotangent, send_order)

    gain_attn = norm_attn.astype(jnp.float32)
    gain_ffn = norm_ffn.astype(jnp.float32)
    parity = my_rank % 2
    where = jnp.stack([my_lane, parity, my_rank]).astype(jnp.int32)
    layouts = [stream_layout(lengths[micro], my_rank, slot_rows) for micro in range(MB)]
    own_segment = jnp.concatenate(
        [
            lax.dynamic_slice_in_dim(one[0], slot_rows + my_lane * micro_rows, micro_rows)
            for one in layouts
        ]
    )
    validity = (own_segment >= 0).astype(jnp.float32)[:, None]
    row_position = jnp.stack(
        [one[1][slot_rows:].reshape(lane_count, micro_rows) for one in layouts], axis=1
    ).reshape(all_rows)
    cosine, sine = (
        one.reshape(lane_count, row_count, 2 * HEAD_DIM) for one in angles(row_position)
    )
    segments = [one[0] for one in layouts]
    by_slot = jnp.where(parity == 0, jnp.stack(segments), jnp.stack(segments[::-1]))
    seg_col = by_slot[:, :, None]
    seg_row = by_slot[:, None, slot_rows:]

    dealt_x = unpack(got_x, recv_place)
    resid = dealt_x.astype(jnp.float32) * validity
    rate_attn = norm_rate(resid)
    attn_in = (resid * rate_attn * gain_attn[None, :]).astype(jnp.bfloat16)
    attn_in = plan.before("norm1", attn_in)
    rows_attn = LaneGather(attn_in, order).finish(order)
    plan.done("norm1", attn_in)
    (got_qkv,) = ring_qkv.gathered()
    rows_attn[0] = plan.before("project", rows_attn[0])
    queries, sent_kv, kept_kv, wqkv, attn_rows = project(
        where, got_qkv, features, rows_attn, cosine, sine
    )
    before = to_next(sent_kv, rank_count, 1)
    plan.done("project", queries)
    out_first, lse_first = attend(
        0, seg_col, seg_row, plan.before("attend1", queries), sent_kv
    )
    plan.done("attend1", out_first)
    if PLAN.get("C") == "attend1":
        got_cot = exchange(after(cotangent, out_first), send_order)
    out_second, lse_second = attend(
        1, seg_col, seg_row, queries, plan.before("attend2", after(kept_kv, out_first)), before
    )
    plan.done("attend2", out_second)
    (got_out,) = ring_out.gathered()
    own, across, pair, attn_out, w_out_full = merge(
        where, got_out, out_first, plan.before("merge", out_second)
    )
    plan.done("merge", pair)
    if PLAN.get("C") == "merge":
        got_cot = exchange(after(cotangent, pair), send_order)
    sum_attn = LaneSum(own, across, pair, order)
    sum_attn.got = plan.before("cross1", sum_attn.got)
    sum_attn.cross(order)
    plan.done("cross1", sum_attn.got)
    if PLAN.get("C") == "cross1":
        got_cot = exchange(after(cotangent, sum_attn.got), send_order)
    order.at()
    middle = resid + BRANCH * sum_attn.finish()
    rate_ffn = norm_rate(middle)
    ffn_in = (middle * rate_ffn * gain_ffn[None, :]).astype(jnp.bfloat16)
    ffn_in = plan.before("norm2", ffn_in)
    gather_ffn = LaneGather(ffn_in, order)
    plan.done("norm2", ffn_in)
    gather_ffn.chip = plan.before("both2", gather_ffn.chip)
    rows_ffn = gather_ffn.finish(order)
    plan.done("both2", gather_ffn.chip)
    dealt_cot = unpack(got_cot, recv_place)
    cot_in = (BRANCH * dealt_cot.astype(jnp.float32)).astype(jnp.bfloat16)
    if PLAN.get("X"):
        cot_in = after(cot_in, {"norm2": ffn_in, "both2": gather_ffn.chip, "merge": pair}[PLAN["X"]])
    gather_cot = LaneGather(cot_in, order)
    gather_cot.finish(order)
    cot_branch = gather_cot.whole()
    (got_gate, got_up) = ring_ffn.gathered()
    rows_ffn[0] = plan.before("hidden", rows_ffn[0])
    gate, upward, hidden, wg, wu, ffn_rows = hidden_units(
        where, got_gate, got_up, rows_ffn
    )
    plan.done("hidden", hidden)
    grad_wd = contract_rows(rows_of(cot_branch), rows_of(plan.before("wd", hidden)))
    plan.add("r", RingSum([grad_wd], rank_count, where))
    plan.done("wd", grad_wd)
    (got_down,) = ring_down.gathered()
    grad_gate, grad_upward, wd = split_grads(
        where, got_down, plan.before("split", after(cot_branch, grad_wd)), gate, upward
    )
    plan.done("split", grad_gate)
    own, across, pair = terms(
        where, [(plan.before("da2", grad_gate), wg), (grad_upward, wu)]
    )
    plan.done("da2", pair)
    sum_grad_ffn = LaneSum(own, across, pair, order)
    grad_wg = contract_rows(
        rows_of(ffn_rows), rows_of(plan.before("wg", after(grad_gate, pair)))
    )
    plan.done("wg", grad_wg)
    sum_grad_ffn.got = plan.before("cross2", after(sum_grad_ffn.got, grad_wg))
    sum_grad_ffn.cross(order)
    order.at()
    grad_wu = contract_rows(
        rows_of(ffn_rows),
        rows_of(plan.before("wu", after(grad_upward, grad_wg, sum_grad_ffn.got))),
    )
    plan.add("e", RingSum([grad_wg, grad_wu], rank_count, where))
    plan.done("wu", grad_wu)
    own, across, pair = terms(where, [(plan.before("yf", after(hidden, grad_wu)), wd)])
    plan.done("yf", pair)
    sum_grad_ffn.far = plan.before("norm3", after(sum_grad_ffn.far, pair))
    plan.done("far3", sum_grad_ffn.far)
    grad_ffn_in = sum_grad_ffn.finish()
    grad_middle = dealt_cot.astype(jnp.float32) + norm_backward(
        grad_ffn_in, middle, rate_ffn, gain_ffn
    )
    grad_branch_in = (BRANCH * grad_middle).astype(jnp.bfloat16)
    gather_branch = LaneGather(plan.before("gather3", grad_branch_in), order)
    plan.done("norm3", gather_branch.block)
    gain_total_ffn = jnp.sum(grad_ffn_in * middle * rate_ffn, axis=0)
    sum_down_out = LaneSum(own, across, after(pair, gather_branch.block), order)
    gather_branch.chip = plan.before("both3", after(gather_branch.chip, sum_down_out.got))
    rows_branch = gather_branch.finish(order)
    plan.done("both3", gather_branch.chip)
    order.at(gather_branch.chip)
    sum_down_out.cross(order)
    order.at()
    rows_branch[0] = plan.before("mixed", rows_branch[0])
    grad_mixed, grad_branch = mixed_grads(where, w_out_full, features, rows_branch)
    plan.done("mixed", grad_mixed)
    late = PLAN.get("W", "wqkv")
    if late == "mixed":
        grad_wo = contract_rows(rows_of(grad_branch), rows_of(after(attn_out, grad_mixed)))
        plan.add("f", RingSum([grad_wo], rank_count, where))
        plan.done("wo", grad_wo)
        grad_mixed = after(grad_mixed, grad_wo)
    *grads_second, shared = attend_back(
        1, seg_col, seg_row, queries, kept_kv, out_second,
        plan.before("back2", grad_mixed), lse_second, before
    )
    back = to_next(shared, rank_count, -1)
    plan.done("back2", shared)
    grads_first = attend_back(
        0, seg_col, seg_row, queries, sent_kv, out_first,
        plan.before(
            "back1", after(grad_mixed, shared, *((sum_down_out.far,) if PLAN.get("P6") else ()))
        ),
        lse_first
    )
    plan.done("back1", grads_first[0])
    if late == "back1":
        grad_wo = contract_rows(rows_of(grad_branch), rows_of(after(attn_out, grads_first[0])))
        plan.add("f", RingSum([grad_wo], rank_count, where))
        plan.done("wo", grad_wo)
        back = after(back, grad_wo)
    output_rows = (middle + BRANCH * sum_down_out.finish()).astype(jnp.bfloat16)
    ready = PLAN.get("O")
    if ready in ("back1", "back2"):
        output_rows = after(output_rows, grads_first[0] if ready == "back1" else shared)
        got_output = exchange(output_rows, back_order)
    grad_qkv = join_grads(
        where, grads_first, grads_second,
        plan.before("join", after(back, grads_first[0])), cosine, sine
    )
    plan.done("join", grad_qkv)
    grad_wqkv = contract_rows(rows_of(attn_rows), rows_of(plan.before("wqkv", grad_qkv)))
    plan.add("u", RingSum([grad_wqkv], rank_count, where))
    plan.done("wqkv", grad_wqkv)
    tail = grad_wqkv
    if late == "wqkv":
        grad_wo = contract_rows(rows_of(grad_branch), rows_of(after(attn_out, grad_wqkv)))
        plan.add("f", RingSum([grad_wo], rank_count, where))
        plan.done("wo", grad_wo)
        tail = grad_wo
    if ready not in ("back1", "back2", "da1"):
        got_output = exchange(after(output_rows, tail), back_order)
    own, across, pair = terms(
        where,
        [
            (
                plan.before(
                    "da1", after(grad_qkv, tail, *((got_output,) if PLAN.get("OL") == "da1" else ()))
                ),
                wqkv,
            )
        ],
    )
    if ready == "da1":
        got_output = exchange(after(output_rows, pair), back_order)
    pair = plan.before("sum4", pair)
    if PLAN.get("OL") == "sum4":
        pair = after(pair, got_output)
    plan.done("da1", pair)
    sum_grad_attn = LaneSum(own, across, pair, order)
    sum_grad_attn.got = plan.before("cross4", sum_grad_attn.got)
    sum_grad_attn.cross(order)
    plan.done("cross4", sum_grad_attn.got)
    sum_grad_attn.far = plan.before("norm4", sum_grad_attn.far)
    grad_attn_in = sum_grad_attn.finish()
    gain_total_attn = jnp.sum(grad_attn_in * resid * rate_attn, axis=0)
    grad_resid = grad_middle + norm_backward(grad_attn_in, resid, rate_attn, gain_attn)
    gains = jnp.stack([gain_total_attn, gain_total_ffn])
    main = gains.astype(jnp.bfloat16)
    rest = (gains - main.astype(jnp.float32)).astype(jnp.bfloat16)
    extra = jnp.concatenate([main, rest, jnp.zeros((BLK - 4, width), jnp.bfloat16)], axis=0)
    got_grad = exchange((validity * grad_resid).astype(jnp.bfloat16), back_order, extra)
    plan.done("norm4", sum_grad_attn.far)
    plan.done("deal", got_grad)
    got_grad = plan.before("unpack", got_grad)
    extra = got_grad[:, per_pair * BLK :].astype(jnp.float32)
    gains = sum_over(jnp.sum(extra[:, :2] + extra[:, 2:4], axis=0), "narrow", lane_count)
    output = unpack(got_output, send_place)
    grad_tokens = unpack(got_grad, send_place)
    (sum_wd,) = plan.rings["r"].finish()
    sum_wg, sum_wu = plan.rings["e"].finish()
    (sum_wo,) = plan.rings["f"].finish()
    (sum_wqkv,) = plan.rings["u"].finish()
    return (
        output,
        grad_tokens,
        gains[0],
        gains[1],
        sum_wqkv[:, :features],
        sum_wqkv[:, features : 2 * features],
        sum_wqkv[:, 2 * features :],
        sum_wo.T,
        sum_wg,
        sum_wu,
        sum_wd.T,
    )


def solution(mesh):
    placed = (
        P(("wide", "narrow"), None),
        P(),
        P(),
        P("wide", "narrow"),
        P("wide", "narrow"),
        P("wide", "narrow"),
        P("narrow", "wide"),
        P("wide", "narrow"),
        P("wide", "narrow"),
        P("narrow", "wide"),
        P(("wide", "narrow"), None),
        P(),
        P(),
    )
    return jax.shard_map(
        body,
        mesh=mesh,
        in_specs=placed,
        out_specs=(
            P(("wide", "narrow"), None),
            P(("wide", "narrow"), None),
            P(),
            P(),
            P("wide", "narrow"),
            P("wide", "narrow"),
            P("wide", "narrow"),
            P("narrow", "wide"),
            P("wide", "narrow"),
            P("wide", "narrow"),
            P("narrow", "wide"),
        ),
        check_vma=False,
    )
```
